128 devices in a mesh: mem: 8 (over z, y_lo), state: 16 (over y_hi, x, core).
Axes of the slice: x: 4, y: 4 (y_hi: 2, y_lo: 2; y = y_hi * 2 + y_lo), z: 4, core: 2. Of those that a mesh axis runs over, the one named last changes fastest.
Arguments:
- anomalies: bfloat16 [128, 32, 65536], P('mem', None, 'state'), may hold values from -0.75 to 0.75
- alpha: bfloat16 [128, 32, 2048], P('mem', None, 'state'), may hold values from -6 to 6
- basis: bfloat16 [2048, 65536], P(None, 'state'), may hold values from -0.1875 to 0.1875
- gradient: bfloat16 [32, 65536], P(None, 'state'), may hold values from -6 to 6
- vertical_root: float32 [32, 32], replicated, may hold values from -1 to 1
- band_gain: float32 [16], replicated, may hold values from 0.25 to 2
- band: int32 [2048], P('state'), may hold values from 0 to 15
- order: int32 [128], replicated, may hold values from 0 to 127, each once
Outputs:
- increment: float32 [32, 65536], P(None, 'state')
- alpha_grad: float32 [128, 32, 2048], P('mem', None, 'state')
The draws below stay inside these ranges and needn't reach their ends.
Inputs may be any that keep to these rules, and one draw needn't show every extreme that they name: `order`: a permutation: every member is named by exactly one slot.
All inputs are finite; a program needn't handle non-finite values.
Results may differ from the reference program's by a relative error of at most 0.0029.
Values may be sent and summed in bfloat16 or wider, within the bound.
A program may use at most 128 MiB of HBM per device.

```python
import math
import jax
import jax.numpy as jnp
from jax import lax

LEVELS = 32
MODES = 2048
BANDS = 16
MEMBERS = 128
COLUMNS = 65536


def set_ends(result, key, least, top_value):
    spot = [jax.random.randint(jax.random.fold_in(key, axis), (), 0, length) for axis, length in enumerate(result.shape)]
    main_axis = result.shape.index(max(result.shape))
    neighbour = spot[:main_axis] + [(spot[main_axis] + 1) % result.shape[main_axis]] + spot[main_axis + 1:]
    return result.at[tuple(spot)].set(least).at[tuple(neighbour)].set(top_value)


def raised(values, key, source, target, blocks, factor):
    owner, partner = [(jnp.arange(values.shape[dim]) // (values.shape[dim] // blocks)).reshape([-1 if axis == dim else 1 for axis in range(values.ndim)]) for dim in (source, target)]
    chosen = jax.random.permutation(key, blocks)[partner]
    strong = (owner == chosen) | (owner == (partner + blocks // 2) % blocks)
    return jnp.where(strong, factor * values, values)


def steps_of(own_key, extent, shards, low, top_value):
    gain, own = 1.0, jax.random.fold_in(own_key, 6)
    for axis_at, parts in shards:
        heights = jnp.exp(jax.random.uniform(jax.random.fold_in(own, axis_at), (parts,), jnp.float32, low / len(shards), top_value / len(shards)))
        gain = gain * jnp.repeat(heights, extent[axis_at] // parts).reshape([-1 if axis == axis_at else 1 for axis in range(len(extent))])
    return gain


def normal_values(own_key, shape, spread, reach, cuts=(), kind=jnp.bfloat16):
    result = jax.random.normal(own_key, shape, jnp.float32) * spread
    if len(cuts) > 0:
        result = steps_of(own_key, shape, cuts, -0.22, 0.18) * result
    return jnp.clip(result, min=-reach, max=reach).astype(kind)


def noise_with(rng, dims, scale, most, pieces, heavy, kind=jnp.bfloat16):
    array = scale * jax.random.normal(rng, dims, jnp.float32)
    if pieces:
        array = array * steps_of(rng, dims, pieces, -0.22, 0.18)
    return jnp.clip(raised(array, jax.random.fold_in(rng, 3), *heavy), -most, most).astype(kind)


def setup_inputs(seed: int = 0) -> dict:
    arg_keys = jax.random.split(jax.random.key(seed), 9)
    return {
        "anomalies": normal_values(arg_keys[0], (MEMBERS, LEVELS, COLUMNS), 0.125, 0.75, ((0, 8), (2, 16))),
        "alpha": normal_values(arg_keys[1], (MEMBERS, LEVELS, MODES), 1.0, 6.0, ((0, 8), (2, 16))),
        "basis": noise_with(arg_keys[2], (MODES, COLUMNS), MODES ** -0.5, 0.1875, ((1, 16),), (1, 0, 16, 2.0)),
        "gradient": normal_values(arg_keys[3], (LEVELS, COLUMNS), 1.0, 6.0, ((1, 16),)),
        "vertical_root": normal_values(arg_keys[4], (LEVELS, LEVELS), LEVELS ** -0.5, 1.0, (), jnp.float32),
        "band_gain": jnp.clip(jnp.exp(jax.random.uniform(arg_keys[5], (BANDS,), jnp.float32, math.log(0.25), math.log(2.0))), 0.25, 2.0),
        "band": set_ends(jax.random.randint(arg_keys[6], (MODES,), 0, BANDS), jax.random.fold_in(arg_keys[6], 1), 0, BANDS - 1).astype(jnp.int32),
        "order": jax.random.permutation(arg_keys[7], MEMBERS).astype(jnp.int32),
    }


def reference(anomalies, alpha, basis, gradient, vertical_root, band_gain, band, order):
    high = lax.Precision.HIGHEST
    onehot = (band[:, None] == jnp.arange(BANDS, dtype=jnp.int32)[None, :]).astype(jnp.float32)
    filter_gain = jnp.sum(onehot * band_gain[None, :], axis=1)
    coef = jnp.einsum("ab,jbk->jak", vertical_root, alpha.astype(jnp.float32), precision=high)
    coef = (coef * filter_gain[None, None, :]).astype(jnp.bfloat16)
    inverse = jnp.zeros((MEMBERS,), jnp.int32).at[order].set(jnp.arange(MEMBERS, dtype=jnp.int32))
    member_coef = coef[inverse]
    grad_float = gradient.astype(jnp.float32)

    def one_member(running, member_items):
        member_anom, member_c = member_items
        member_field = jnp.dot(member_c, basis, preferred_element_type=jnp.float32)
        running = running + member_anom.astype(jnp.float32) * member_field
        weighted = (member_anom.astype(jnp.float32) * grad_float).astype(jnp.bfloat16)
        projected = lax.dot_general(weighted, basis, (((1,), (1,)), ((), ())), preferred_element_type=jnp.float32)
        return running, projected

    increment, projected = lax.scan(one_member, jnp.zeros((LEVELS, COLUMNS), jnp.float32), (anomalies, member_coef))
    slot_proj = projected[order]
    alpha_grad = jnp.einsum("ab,jak->jbk", vertical_root, slot_proj, precision=high) * filter_gain[None, None, :]
    return increment, alpha_grad
```

```python
import functools

import jax
import jax.numpy as jnp
from jax import lax
from jax.experimental import pallas as pl
from jax.experimental.pallas import tpu as pltpu
from jax.sharding import PartitionSpec as P

MESH = pl.DeviceIdType.MESH
NT = (((1,), (1,)), ((), ()))
HIGH = lax.Precision.HIGHEST
F32 = jnp.float32
BF16 = jnp.bfloat16


def kernel(
    order, inverse, gains, anom_hbm, alpha, basis_hbm, grad, root, band,
    inc_out, ag_out,
    basis, anom, weighted, part, half, outgo, landed, coefs, zall, ypart, ysend,
    inc_acc, inc_send, inc_land, inc_own, gall, gpart, gsend,
    load_sem, asem, z_s, z_r, y_s, y_r, b_s, b_r, d_s, d_r, x_s, x_r, r_s, r_r,
    i_s, i_r, o_s, o_r, gz_s, gz_r, gy_s, gy_r,
):
    m = lax.axis_index("mem")
    s = lax.axis_index("state")
    z, yl = m // 2, m % 2
    chip, core = s // 2, s % 2
    yh, x = chip // 4, chip % 4
    other = 1 - core

    def chip_at(t):
        return ((yh + t // 4) % 2) * 4 + (x + t % 4) % 4

    def mem_at(u):
        return ((z + u // 2) % 4) * 2 + (yl + u % 2) % 2

    def back(t):
        return (t // 4) * 4 + (4 - t % 4) % 4

    def remote(src, dst, send, recv, mem, state):
        return pltpu.make_async_remote_copy(
            src_ref=src, dst_ref=dst, send_sem=send, recv_sem=recv,
            device_id=(mem, state), device_id_type=MESH,
        )

    def lanes(start, width):
        return pl.ds(pl.multiple_of(start, 128), width)

    partner = chip * 2 + other
    ymate = z * 2 + (1 - yl)

    def load(r):
        q = chip_at(7 - r)
        return pltpu.make_async_copy(
            basis_hbm.at[pl.ds(pl.multiple_of(q * 256, 256), 256), :],
            basis.at[pl.ds(pl.multiple_of(r * 256, 256), 256), :],
            load_sem.at[r],
        )

    def load_anom(g):
        rows = pl.ds(g * 128, 128)
        return pltpu.make_async_copy(anom_hbm.at[rows, :], anom.at[rows, :], asem.at[g])

    for g in range(4):
        load_anom(g).start()
    load(0).start()
    load(1).start()

    barrier = pltpu.get_barrier_semaphore()
    for u in range(1, 8):
        pl.semaphore_signal(barrier, inc=1, device_id=(mem_at(u), s), device_id_type=MESH)
        pl.semaphore_signal(
            barrier, inc=1, device_id=(m, chip_at(u) * 2 + core), device_id_type=MESH
        )
    pl.semaphore_signal(barrier, inc=1, device_id=(m, partner), device_id_type=MESH)

    bands = band[...]
    gain = jnp.zeros((1, 128), F32)
    for b in range(16):
        gain = jnp.where(bands == b, gains[b], gain)
    rooted = jnp.concatenate([root[...]] * 4, axis=0)
    rooted = jnp.concatenate([rooted] * 4, axis=1)
    row = lax.broadcasted_iota(jnp.int32, (128, 128), 0) // 32
    col = lax.broadcasted_iota(jnp.int32, (128, 128), 1) // 32
    rooted = jnp.where(row == col, rooted, 0.0)
    for g in range(4):
        block = alpha[g * 4:(g + 1) * 4].astype(F32).reshape(128, 128)
        value = jnp.dot(rooted, block, precision=HIGH, preferred_element_type=F32) * gain
        zall[pl.ds(z * 16 + g * 4, 4)] = value.astype(BF16).reshape(4, 32, 128)

    pl.semaphore_wait(barrier, 15)

    def z_copy(all_ref, dz, send, recv, got):
        mine = all_ref.at[pl.ds(z * 16, 16)]
        dst = all_ref.at[pl.ds(((z + 4 - dz) % 4) * 16, 16)] if got else mine
        return remote(mine, dst, send.at[dz - 1], recv.at[dz - 1], ((z + dz) % 4) * 2 + yl, s)

    for dz in (1, 3, 2):
        z_copy(zall, dz, z_s, z_r, False).start()

    for g in range(4):
        load_anom(g).wait()

        def weigh(c, carry):
            w = lanes(c * 512, 512)
            factor = grad[:, w].astype(F32)
            for k in range(4):
                rows = pl.ds(g * 128 + k * 32, 32)
                weighted[rows, w] = (anom[rows, w].astype(F32) * factor).astype(BF16)
            return carry

        lax.fori_loop(0, 8, weigh, 0)

    def pick(table, all_ref, slot):
        where = table[slot]
        same = (where // 16) % 2 == yl
        return same, all_ref[(where // 32) * 16 + where % 16]

    def y_copy(src, dst, send, recv):
        return remote(src, dst, send.at[0], recv.at[0], ymate, s)

    def b_block(r):
        return coefs.at[:, lanes(r * 256 + core * 128, 128)]

    def b_copy(t):
        return remote(
            b_block(7), b_block(7 - back(t)), b_s.at[7 - t], b_r.at[7 - back(t)],
            m, chip_at(t) * 2 + core,
        )

    def d_copy(r):
        return remote(b_block(r), b_block(r), d_s.at[r], d_r.at[r], m, partner)

    def d_got(r):
        there = coefs.at[:, lanes(r * 256 + other * 128, 128)]
        return remote(there, there, d_s.at[r], d_r.at[r], m, partner)

    def x_copy(r):
        return remote(
            part.at[r, :, lanes(other * 128, 128)], half.at[r], x_s.at[r], x_r.at[r], m, partner
        )

    def r_copy(r):
        return remote(
            outgo.at[r], landed.at[r], r_s.at[r], r_r.at[r], m, chip_at(7 - r) * 2 + core
        )

    def adjoint(r, carry):
        @pl.when(r < 6)
        def _():
            load(r + 2).start()

        load(r).wait()
        rows = pl.ds(pl.multiple_of(r * 256, 256), 256)
        part[r] = lax.dot_general(weighted[...], basis[rows, :], NT, preferred_element_type=F32)
        x_copy(r).start()

        @pl.when(r > 0)
        def _():
            p = r - 1
            x_copy(p).wait_recv()
            outgo[p] = (part[p, :, lanes(core * 128, 128)] + half[p]).astype(BF16)
            r_copy(p).start()

        @pl.when(r == 3)
        def _():
            for dz in (1, 3, 2):
                z_copy(zall, dz, z_s, z_r, True).wait_recv()
            for i in range(16):
                same, value = pick(inverse, zall, ymate * 16 + i)
                ysend[i] = jnp.where(same, value, jnp.zeros_like(value))
            y_copy(ysend, ypart, y_s, y_r).start()

        @pl.when(r == 5)
        def _():
            y_copy(ysend, ypart, y_s, y_r).wait_recv()
            for i in range(16):
                same, value = pick(inverse, zall, m * 16 + i)
                coefs[pl.ds(i * 32, 32), lanes(7 * 256 + core * 128, 128)] = jnp.where(
                    same, value, ypart[i]
                )
            d_copy(7).start()
            for t in (1, 3, 2, 4, 5, 7, 6):
                b_copy(t).start()

        return carry

    lax.fori_loop(0, 8, adjoint, 0)

    def b_got(r):
        return remote(b_block(r), b_block(r), b_s.at[r], b_r.at[r], m, s)

    def pass_on(r):
        remote(
            b_block(7), b_block(r), b_s.at[r], b_r.at[r], m, chip_at(7 - r) * 2 + core
        ).wait_recv()
        d_copy(r).start()

    def field_part(low, c):
        w = lanes(c * 512, 512)
        f = jnp.dot(coefs[:, low:low + 1024], basis[low:low + 1024, w], preferred_element_type=F32)
        return w, jnp.sum((f * anom[:, w].astype(F32)).reshape(16, 32, 512), axis=0)

    for r in (4, 5, 6):
        pass_on(r)
    for r in (7, 4, 5, 6):
        d_got(r).wait_recv()

    def near(c, carry):
        w, value = field_part(1024, c)
        inc_acc[:, w] = value

        @pl.when(c == 4)
        def _():
            for r in range(4):
                pass_on(r)

        return carry

    lax.fori_loop(0, 8, near, 0)

    x_copy(7).wait_recv()
    for r in range(7):
        r_copy(r).wait_recv()
    for g in range(4):
        rows = pl.ds(g * 128, 128)
        total = part[7, rows, lanes(core * 128, 128)] + half[7, rows, :]
        for r in range(7):
            total = total + landed[r, rows, :].astype(F32)
        value = jnp.dot(rooted.T, total, precision=HIGH, preferred_element_type=F32) * gain
        gall[pl.ds(z * 16 + g * 4, 4)] = value.astype(BF16).reshape(4, 32, 128)
    for dz in (1, 3, 2):
        z_copy(gall, dz, gz_s, gz_r, False).start()

    for r in range(4):
        d_got(r).wait_recv()

    def i_copy(i):
        return remote(inc_send.at[i], inc_land.at[i], i_s.at[i], i_r.at[i], mem_at(7 - i), s)

    def far(i, carry):
        w, value = field_part(0, mem_at(7 - i))
        inc_send[i] = value + inc_acc[:, w]

        @pl.when(i < 7)
        def _():
            i_copy(i).start()

        @pl.when(i == 5)
        def _():
            for dz in (1, 3, 2):
                z_copy(gall, dz, gz_s, gz_r, True).wait_recv()
            for k in range(16):
                same, got = pick(order, gall, ymate * 16 + k)
                gsend[k] = jnp.where(same, got, jnp.zeros_like(got))
            y_copy(gsend, gpart, gy_s, gy_r).start()

        return carry

    lax.fori_loop(0, 8, far, 0)

    total = inc_send[7]
    for i in range(7):
        i_copy(i).wait_recv()
        total = total + inc_land[i]
    inc_own[...] = total

    def o_copy(u, got):
        target = mem_at(u)
        spot = mem_at(((4 - u // 2) % 4) * 2 + u % 2) if got else m
        return remote(
            inc_own, inc_out.at[:, lanes(spot * 512, 512)], o_s.at[u - 1], o_r.at[u - 1], target, s
        )

    for u in (4, 5, 1, 2, 3, 6, 7):
        o_copy(u, False).start()
    inc_out[:, lanes(m * 512, 512)] = total

    y_copy(gsend, gpart, gy_s, gy_r).wait_recv()
    for i in range(16):
        same, value = pick(order, gall, m * 16 + i)
        ag_out[i] = jnp.where(same, value, gpart[i]).astype(F32)

    for u in range(1, 8):
        o_copy(u, True).wait_recv()

    for dz in (1, 2, 3):
        z_copy(zall, dz, z_s, z_r, False).wait_send()
        z_copy(gall, dz, gz_s, gz_r, False).wait_send()
    y_copy(ysend, ypart, y_s, y_r).wait_send()
    y_copy(gsend, gpart, gy_s, gy_r).wait_send()
    for t in range(1, 8):
        b_copy(t).wait_send()
        r_copy(t - 1).wait_send()
        i_copy(t - 1).wait_send()
        o_copy(t, False).wait_send()
    for r in range(8):
        d_copy(r).wait_send()
        x_copy(r).wait_send()


def on_device(anomalies, alpha, basis, gradient, vertical_root, band_gain, band, order):
    members, levels, columns = anomalies.shape
    slots = jnp.arange(order.shape[0], dtype=jnp.int32)
    inverse = jnp.sum(jnp.where(order[None, :] == slots[:, None], slots[None, :], 0), axis=1)
    vmem, smem = pl.BlockSpec(memory_space=pltpu.VMEM), pl.BlockSpec(memory_space=pltpu.SMEM)
    hbm = pl.BlockSpec(memory_space=pl.ANY)
    dma = lambda n: pltpu.SemaphoreType.DMA((n,))
    return pl.pallas_call(
        kernel,
        out_shape=(
            jax.ShapeDtypeStruct((32, 4096), F32),
            jax.ShapeDtypeStruct((16, 32, 128), F32),
        ),
        in_specs=[smem, smem, smem, hbm, vmem, hbm, vmem, vmem, vmem],
        out_specs=(vmem, vmem),
        scratch_shapes=[
            pltpu.VMEM((2048, 4096), BF16),
            pltpu.VMEM((512, 4096), BF16),
            pltpu.VMEM((512, 4096), BF16),
            pltpu.VMEM((8, 512, 256), F32),
            pltpu.VMEM((8, 512, 128), F32),
            pltpu.VMEM((7, 512, 128), BF16),
            pltpu.VMEM((7, 512, 128), BF16),
            pltpu.VMEM((512, 2048), BF16),
            pltpu.VMEM((64, 32, 128), BF16),
            pltpu.VMEM((16, 32, 128), BF16),
            pltpu.VMEM((16, 32, 128), BF16),
            pltpu.VMEM((32, 4096), F32),
            pltpu.VMEM((8, 32, 512), F32),
            pltpu.VMEM((7, 32, 512), F32),
            pltpu.VMEM((32, 512), F32),
            pltpu.VMEM((64, 32, 128), BF16),
            pltpu.VMEM((16, 32, 128), BF16),
            pltpu.VMEM((16, 32, 128), BF16),
            dma(8), dma(4), dma(3), dma(3), dma(1), dma(1), dma(7), dma(7), dma(8), dma(8),
            dma(8), dma(8), dma(7), dma(7), dma(7), dma(7), dma(7), dma(7), dma(3), dma(3),
            dma(1), dma(1),
        ],
        compiler_params=pltpu.CompilerParams(
            collective_id=0, has_side_effects=True, vmem_limit_bytes=60 << 20
        ),
    )(
        order, inverse, band_gain, anomalies.reshape(members * levels, columns), alpha, basis,
        gradient, vertical_root, band.reshape(1, -1),
    )


def solution(mesh):
    return jax.shard_map(
        on_device,
        mesh=mesh,
        in_specs=(
            P("mem", None, "state"),
            P("mem", None, "state"),
            P(None, "state"),
            P(None, "state"),
            P(),
            P(),
            P("state"),
            P(),
        ),
        out_specs=(P(None, "state"), P("mem", None, "state")),
        check_vma=False,
    )
```

```python
import functools

import jax
import jax.numpy as jnp
from jax import lax
from jax.experimental import pallas as pl
from jax.experimental.pallas import tpu as pltpu
from jax.sharding import PartitionSpec as P

MESH = pl.DeviceIdType.MESH
NT = (((1,), (1,)), ((), ()))
HIGH = lax.Precision.HIGHEST
F32 = jnp.float32
BF16 = jnp.bfloat16


def kernel(
    order, inverse, gains, anom_hbm, alpha, basis_hbm, grad, root, band,
    inc_out, ag_out,
    basis, anom, weighted, part, half, outgo, landed, rsend, rland, coefs, zall0, zall1, ypart, ysend,
    inc_acc, inc_send, inc_land, inc_own, inc_all, gall0, gall1, gpart, gsend,
    load_sem, asem, z_s, z_r, y_s, y_r, q_s, q_r, px_s, px_r, py_s, py_r, d_s, d_r, x_s, x_r,
    r_s, r_r, ry_s, ry_r, i_s, i_r, o_s, o_r, gz_s, gz_r, gy_s, gy_r,
):
    zall, gall = (zall0, zall1), (gall0, gall1)
    m = lax.axis_index("mem")
    s = lax.axis_index("state")
    z, yl = m // 2, m % 2
    chip, core = s // 2, s % 2
    yh, x = chip // 4, chip % 4
    other = 1 - core

    def chip_at(t):
        return ((yh + t // 4) % 2) * 4 + (x + t % 4) % 4

    def mem_at(u):
        return ((z + u // 2) % 4) * 2 + (yl + u % 2) % 2

    def back(t):
        return (t // 4) * 4 + (4 - t % 4) % 4

    def remote(src, dst, send, recv, mem, state):
        return pltpu.make_async_remote_copy(
            src_ref=src, dst_ref=dst, send_sem=send, recv_sem=recv,
            device_id=(mem, state), device_id_type=MESH,
        )

    def lanes(start, width):
        return pl.ds(pl.multiple_of(start, 128), width)

    partner = chip * 2 + other
    ymate = z * 2 + (1 - yl)

    def load(r):
        q = chip_at(7 - r)
        return pltpu.make_async_copy(
            basis_hbm.at[pl.ds(pl.multiple_of(q * 256, 256), 256), :],
            basis.at[pl.ds(pl.multiple_of(r * 256, 256), 256), :],
            load_sem.at[r],
        )

    def load_anom(g):
        rows = pl.ds(g * 128, 128)
        return pltpu.make_async_copy(anom_hbm.at[rows, :], anom.at[rows, :], asem.at[g])

    for g in range(4):
        load_anom(g).start()
    load(0).start()
    load(1).start()

    barrier = pltpu.get_barrier_semaphore()
    for u in range(1, 8):
        pl.semaphore_signal(barrier, inc=1, device_id=(mem_at(u), s), device_id_type=MESH)
    for t in range(1, 5):
        pl.semaphore_signal(
            barrier, inc=1, device_id=(m, chip_at(t) * 2 + core), device_id_type=MESH
        )
    pl.semaphore_signal(barrier, inc=1, device_id=(m, partner), device_id_type=MESH)

    bands = band[...]
    gain = jnp.zeros((1, 128), F32)
    for b in range(16):
        gain = jnp.where(bands == b, gains[b], gain)
    rooted = jnp.concatenate([root[...]] * 4, axis=0)
    rooted = jnp.concatenate([rooted] * 4, axis=1)
    row = lax.broadcasted_iota(jnp.int32, (128, 128), 0) // 32
    col = lax.broadcasted_iota(jnp.int32, (128, 128), 1) // 32
    rooted = jnp.where(row == col, rooted, 0.0)
    def spread(halves, g, value):
        value = value.astype(BF16).reshape(4, 32, 128)
        for h in range(2):
            halves[h][pl.ds(z * 16 + g * 4, 4)] = value[:, h * 16:(h + 1) * 16, :]

    for g in range(4):
        block = alpha[g * 4:(g + 1) * 4].astype(F32).reshape(128, 128)
        value = jnp.dot(rooted, block, precision=HIGH, preferred_element_type=F32) * gain
        spread(zall, g, value)

    with jax.named_scope('bar'):
        pl.semaphore_wait(barrier, 12)

    def z_copy(all_ref, h, dz, send, recv, got):
        mine = all_ref[h].at[pl.ds(z * 16, 16)]
        dst = all_ref[h].at[pl.ds(((z + 4 - dz) % 4) * 16, 16)] if got else mine
        k = h * 3 + dz - 1
        return remote(mine, dst, send.at[k], recv.at[k], ((z + dz) % 4) * 2 + yl, s)

    for h in range(2):
        for dz in (1, 3, 2):
            z_copy(zall, h, dz, z_s, z_r, False).start()

    for g in range(4):
        with jax.named_scope('anomwait'):
            load_anom(g).wait()

        def weigh(c, carry):
            w = lanes(c * 512, 512)
            factor = grad[:, w].astype(F32)
            for k in range(4):
                rows = pl.ds(g * 128 + k * 32, 32)
                weighted[rows, w] = (anom[rows, w].astype(F32) * factor).astype(BF16)
            return carry

        lax.fori_loop(0, 8, weigh, 0)

    def pick(table, all_ref, h, slot):
        where = table[slot]
        same = (where // 16) % 2 == yl
        return same, all_ref[h][(where // 32) * 16 + where % 16]

    def y_copy(src, dst, h, send, recv):
        levels = pl.ds(h * 16, 16)
        return remote(
            src.at[:, levels], dst.at[:, levels], send.at[h], recv.at[h], ymate, s
        )

    def exchange(table, all_ref, src, dst, h, zs, zr, ys, yr):
        for dz in (1, 3, 2):
            z_copy(all_ref, h, dz, zs, zr, True).wait_recv()
        for i in range(16):
            same, value = pick(table, all_ref, h, ymate * 16 + i)
            src[i, pl.ds(h * 16, 16), :] = jnp.where(same, value, jnp.zeros_like(value))
        y_copy(src, dst, h, ys, yr).start()

    def block(r, h, c):
        return coefs.at[:, pl.ds(h * 16, 16), lanes(r * 256 + c * 128, 128)]

    def b_copy(source, target, h, t, send, recv):
        return remote(
            block(source, h, core), block(target, h, core), send, recv,
            m, chip_at(t) * 2 + core,
        )

    def q_y():
        return b_copy(7, 3, 0, 4, q_s.at[0], q_r.at[0])

    def q_x(dx):
        return b_copy(7, 3 + dx, 0, dx, q_s.at[dx], q_r.at[4 - dx])

    def q_m(dx):
        return b_copy(3, dx - 1, 0, dx, q_s.at[3 + dx], q_r.at[7 - dx])

    def p_x(dx):
        return b_copy(7, 3 + dx, 1, dx, px_s.at[dx - 1], px_r.at[3 - dx])

    def p_y(dx):
        return b_copy(7 - dx, 3 - dx, 1, 4, py_s.at[dx], py_r.at[dx])

    def b_got(r, h, recv):
        here = block(r, h, core)
        return remote(here, here, q_s.at[0], recv, m, chip_at(4) * 2 + core)

    def d_copy(r, h):
        here = block(r, h, core)
        return remote(here, here, d_s.at[2 * r + h], d_r.at[2 * r + h], m, partner)

    def d_got(r, h):
        there = block(r, h, other)
        return remote(there, there, d_s.at[2 * r + h], d_r.at[2 * r + h], m, partner)

    def settle(h):
        y_copy(ysend, ypart, h, y_s, y_r).wait_recv()
        for i in range(16):
            same, value = pick(inverse, zall, h, m * 16 + i)
            coefs[i, pl.ds(h * 16, 16), lanes(7 * 256 + core * 128, 128)] = jnp.where(
                same, value, ypart[i, pl.ds(h * 16, 16), :]
            )

    def x_copy(r):
        return remote(
            part.at[r, :, lanes(other * 128, 128)], half.at[r], x_s.at[r], x_r.at[r], m, partner
        )

    def r_copy(r):
        return remote(
            outgo.at[r], landed.at[r], r_s.at[r], r_r.at[r], m,
            chip_at((7 - r) % 4) * 2 + core,
        )

    def ry_copy():
        return remote(rsend, rland, ry_s.at[0], ry_r.at[0], m, chip_at(4) * 2 + core)

    def own(r, rows):
        return part[r, rows, lanes(core * 128, 128)] + half[r, rows, :]

    def adjoint(r, carry):
        @pl.when(r < 6)
        def _():
            load(r + 2).start()

        with jax.named_scope('bwait'):
            load(r).wait()
        rows = pl.ds(pl.multiple_of(r * 256, 256), 256)
        with jax.named_scope('adot'):
            part[r] = lax.dot_general(weighted[...], basis[rows, :], NT, preferred_element_type=F32)
        x_copy(r).start()

        @pl.when(r > 0)
        def _():
            p = r - 1
            with jax.named_scope('xwait'):
                x_copy(p).wait_recv()

            @pl.when(p != 3)
            def _():
                outgo[p] = (part[p, :, lanes(core * 128, 128)] + half[p]).astype(BF16)
                r_copy(p).start()

        @pl.when(r == 2)
        def _():
            with jax.named_scope('zwait'):
                exchange(inverse, zall, ysend, ypart, 0, z_s, z_r, y_s, y_r)

        @pl.when(r == 4)
        def _():
            with jax.named_scope('zwait'):
                exchange(inverse, zall, ysend, ypart, 1, z_s, z_r, y_s, y_r)

        @pl.when(r == 5)
        def _():
            with jax.named_scope('ywait'):
                settle(0)
            q_y().start()
            for dx in (1, 3, 2):
                q_x(dx).start()

        @pl.when(r == 6)
        def _():
            with jax.named_scope('ywait'):
                settle(1)
            p_y(0).start()
            for dx in (1, 3, 2):
                p_x(dx).start()
            for h in range(2):
                d_copy(7, h).start()

        return carry

    lax.fori_loop(0, 8, adjoint, 0)

    with jax.named_scope('qywait'):
        b_got(3, 0, q_r.at[0]).wait_recv()
    for dx in (1, 3, 2):
        q_m(dx).start()
    d_copy(3, 0).start()

    for r in range(3):
        with jax.named_scope('rfwait'):
            r_copy(r).wait_recv()
    for g in range(4):
        rows = pl.ds(g * 128, 128)
        total = own(3, rows)
        for r in range(3):
            total = total + landed[r, rows, :].astype(F32)
        rsend[rows, :] = total
    ry_copy().start()

    for dx in (1, 3, 2):
        with jax.named_scope('qxwait'):
            b_got(7 - dx, 0, q_r.at[dx]).wait_recv()
        d_copy(7 - dx, 0).start()
    for dx in (1, 3, 2):
        with jax.named_scope('pxwait'):
            b_got(7 - dx, 1, px_r.at[dx - 1]).wait_recv()
        p_y(dx).start()
        d_copy(7 - dx, 1).start()

    def field_part(low, c):
        w = lanes(c * 512, 512)
        f = jnp.dot(
            coefs[:, :, low:low + 1024].reshape(512, 1024), basis[low:low + 1024, w],
            preferred_element_type=F32,
        )
        return w, jnp.sum((f * anom[:, w].astype(F32)).reshape(16, 32, 512), axis=0)

    for r in (7, 6, 4, 5):
        for h in range(2):
            with jax.named_scope('dwait'):
                d_got(r, h).wait_recv()

    def near(c, carry):
        with jax.named_scope('near'):
            w, value = field_part(1024, c)
        inc_acc[:, w] = value

        @pl.when(c == 1)
        def _():
            with jax.named_scope('rnwait'):
                x_copy(7).wait_recv()
                for r in range(4, 7):
                    r_copy(r).wait_recv()
                ry_copy().wait_recv()
            for g in range(4):
                rows = pl.ds(g * 128, 128)
                total = own(7, rows) + rland[rows, :]
                for r in range(4, 7):
                    total = total + landed[r, rows, :].astype(F32)
                value = jnp.dot(rooted.T, total, precision=HIGH, preferred_element_type=F32) * gain
                spread(gall, g, value)
            for h in range(2):
                for dz in (1, 3, 2):
                    z_copy(gall, h, dz, gz_s, gz_r, False).start()

        @pl.when(c == 4)
        def _():
            for dx in (1, 3, 2):
                with jax.named_scope('qmwait'):
                    b_got(3 - dx, 0, q_r.at[3 + dx]).wait_recv()
                d_copy(3 - dx, 0).start()
            for dx in (0, 1, 3, 2):
                with jax.named_scope('pywait'):
                    b_got(3 - dx, 1, py_r.at[dx]).wait_recv()
                d_copy(3 - dx, 1).start()

        return carry

    lax.fori_loop(0, 8, near, 0)

    for r in range(4):
        for h in range(2):
            with jax.named_scope('fdwait'):
                d_got(r, h).wait_recv()

    def i_copy(i):
        return remote(inc_send.at[i], inc_land.at[i], i_s.at[i], i_r.at[i], mem_at(7 - i), s)

    def far(i, carry):
        with jax.named_scope('far'):
            w, value = field_part(0, mem_at(7 - i))
        inc_send[i] = (value + inc_acc[:, w]).astype(BF16)

        @pl.when(i < 7)
        def _():
            i_copy(i).start()

        @pl.when(i == 2)
        def _():
            with jax.named_scope('gzwait'):
                exchange(order, gall, gsend, gpart, 0, gz_s, gz_r, gy_s, gy_r)

        @pl.when(i == 4)
        def _():
            with jax.named_scope('gzwait'):
                exchange(order, gall, gsend, gpart, 1, gz_s, gz_r, gy_s, gy_r)

        return carry

    lax.fori_loop(0, 8, far, 0)

    total = inc_send[7].astype(F32)
    for i in range(7):
        with jax.named_scope(f'iwait{i}'):
            i_copy(i).wait_recv()
        total = total + inc_land[i].astype(F32)
    inc_own[...] = total.astype(BF16)

    def o_copy(u, got):
        target = mem_at(u)
        spot = mem_at(((4 - u // 2) % 4) * 2 + u % 2) if got else m
        return remote(
            inc_own, inc_all.at[spot], o_s.at[u - 1], o_r.at[u - 1], target, s
        )

    for u in (4, 5, 1, 2, 3, 6, 7):
        o_copy(u, False).start()
    inc_out[:, lanes(m * 512, 512)] = inc_own[...].astype(F32)

    for h in range(2):
        with jax.named_scope('gywait'):
            y_copy(gsend, gpart, h, gy_s, gy_r).wait_recv()
        for i in range(16):
            same, value = pick(order, gall, h, m * 16 + i)
            levels = pl.ds(h * 16, 16)
            ag_out[i, levels, :] = jnp.where(same, value, gpart[i, levels, :]).astype(F32)

    for u in range(1, 8):
        with jax.named_scope('owait'):
            o_copy(u, True).wait_recv()
        spot = mem_at(((4 - u // 2) % 4) * 2 + u % 2)
        inc_out[:, lanes(spot * 512, 512)] = inc_all[spot].astype(F32)

    for h in range(2):
        for dz in (1, 2, 3):
            z_copy(zall, h, dz, z_s, z_r, False).wait_send()
            z_copy(gall, h, dz, gz_s, gz_r, False).wait_send()
        y_copy(ysend, ypart, h, y_s, y_r).wait_send()
        y_copy(gsend, gpart, h, gy_s, gy_r).wait_send()
    q_y().wait_send()
    p_y(0).wait_send()
    for dx in (1, 2, 3):
        q_x(dx).wait_send()
        q_m(dx).wait_send()
        p_x(dx).wait_send()
        p_y(dx).wait_send()
    for r in (0, 1, 2, 4, 5, 6):
        r_copy(r).wait_send()
    ry_copy().wait_send()
    for t in range(1, 8):
        i_copy(t - 1).wait_send()
        o_copy(t, False).wait_send()
    for r in range(8):
        x_copy(r).wait_send()
        for h in range(2):
            d_copy(r, h).wait_send()


def on_device(anomalies, alpha, basis, gradient, vertical_root, band_gain, band, order):
    members, levels, columns = anomalies.shape
    slots = jnp.arange(order.shape[0], dtype=jnp.int32)
    inverse = jnp.sum(jnp.where(order[None, :] == slots[:, None], slots[None, :], 0), axis=1)
    vmem, smem = pl.BlockSpec(memory_space=pltpu.VMEM), pl.BlockSpec(memory_space=pltpu.SMEM)
    hbm = pl.BlockSpec(memory_space=pl.ANY)
    dma = lambda n: pltpu.SemaphoreType.DMA((n,))
    return pl.pallas_call(
        kernel,
        out_shape=(
            jax.ShapeDtypeStruct((32, 4096), F32),
            jax.ShapeDtypeStruct((16, 32, 128), F32),
        ),
        in_specs=[smem, smem, smem, hbm, vmem, hbm, vmem, vmem, vmem],
        out_specs=(vmem, vmem),
        scratch_shapes=[
            pltpu.VMEM((2048, 4096), BF16),
            pltpu.VMEM((512, 4096), BF16),
            pltpu.VMEM((512, 4096), BF16),
            pltpu.VMEM((8, 512, 256), F32),
            pltpu.VMEM((8, 512, 128), F32),
            pltpu.VMEM((7, 512, 128), BF16),
            pltpu.VMEM((7, 512, 128), BF16),
            pltpu.VMEM((512, 128), F32),
            pltpu.VMEM((512, 128), F32),
            pltpu.VMEM((16, 32, 2048), BF16),
            pltpu.VMEM((64, 16, 128), BF16),
            pltpu.VMEM((64, 16, 128), BF16),
            pltpu.VMEM((16, 32, 128), BF16),
            pltpu.VMEM((16, 32, 128), BF16),
            pltpu.VMEM((32, 4096), F32),
            pltpu.VMEM((8, 32, 512), BF16),
            pltpu.VMEM((7, 32, 512), BF16),
            pltpu.VMEM((32, 512), BF16),
            pltpu.VMEM((8, 32, 512), BF16),
            pltpu.VMEM((64, 16, 128), BF16),
            pltpu.VMEM((64, 16, 128), BF16),
            pltpu.VMEM((16, 32, 128), BF16),
            pltpu.VMEM((16, 32, 128), BF16),
            dma(8), dma(4), dma(6), dma(6), dma(2), dma(2), dma(7), dma(7), dma(3), dma(3),
            dma(4), dma(4), dma(16), dma(16), dma(8), dma(8), dma(7), dma(7), dma(1), dma(1),
            dma(7), dma(7), dma(7), dma(7), dma(6), dma(6), dma(2), dma(2),
        ],
        compiler_params=pltpu.CompilerParams(
            collective_id=0, has_side_effects=True, vmem_limit_bytes=60 << 20
        ),
    )(
        order, inverse, band_gain, anomalies.reshape(members * levels, columns), alpha, basis,
        gradient, vertical_root, band.reshape(1, -1),
    )


def solution(mesh):
    return jax.shard_map(
        on_device,
        mesh=mesh,
        in_specs=(
            P("mem", None, "state"),
            P("mem", None, "state"),
            P(None, "state"),
            P(None, "state"),
            P(),
            P(),
            P("state"),
            P(),
        ),
        out_specs=(P(None, "state"), P("mem", None, "state")),
        check_vma=False,
    )
```

```python
import jax
import jax.numpy as jnp
from jax import lax
from jax.experimental import pallas as pl
from jax.experimental.pallas import tpu as pltpu
from jax.sharding import PartitionSpec as P

MESH = pl.DeviceIdType.MESH
NT = (((1,), (1,)), ((), ()))
HIGH = lax.Precision.HIGHEST
F32 = jnp.float32
BF16 = jnp.bfloat16
scope = jax.named_scope


def kernel(
    order_hbm, gains_hbm, anom_hbm, alpha_hbm, basis_hbm, grad_hbm, root_hbm, band_hbm,
    inc_out, ag_out,
    order_v, order, inverse_v, inverse, gains, alpha, grad, root, band,
    basis, anom, weighted, part, half, outgo, landed, rsend, rland, coefs0, coefs1,
    zall0, zall1, ypart, ysend, inc_acc, inc_send, inc_land, inc_own, inc_all, gall0, gall1, gpart, gsend,
    small_sem, load_sem, asem, z_s, z_r, y_s, y_r, b_s, mate_r, row_r, rest_r, d_s, d_r, x_s, x_r,
    r_s, r_r, ry_s, ry_r, i_s, i_r, o_s, o_r, gz_s, gz_r, gy_s, gy_r,
):
    zall, gall, coefs = (zall0, zall1), (gall0, gall1), (coefs0, coefs1)
    m = lax.axis_index("mem")
    s = lax.axis_index("state")
    z, yl = m // 2, m % 2
    chip, core = s // 2, s % 2
    yh, x = chip // 4, chip % 4
    other = 1 - core

    def chip_at(t):
        return ((yh + t // 4) % 2) * 4 + (x + t % 4) % 4

    def mem_at(u):
        return ((z + u // 2) % 4) * 2 + (yl + u % 2) % 2

    def remote(src, dst, send, recv, mem, state):
        return pltpu.make_async_remote_copy(
            src_ref=src, dst_ref=dst, send_sem=send, recv_sem=recv,
            device_id=(mem, state), device_id_type=MESH,
        )

    def wait_all(ref, sem):
        pltpu.make_async_copy(ref, ref, sem).wait()

    def lanes(start, width):
        return pl.ds(pl.multiple_of(start, 128), width)

    partner = chip * 2 + other
    ymate = z * 2 + (1 - yl)

    barrier = pltpu.get_barrier_semaphore()
    for u in range(1, 8):
        pl.semaphore_signal(barrier, inc=1, device_id=(mem_at(u), s), device_id_type=MESH)
    for t in range(1, 5):
        pl.semaphore_signal(
            barrier, inc=1, device_id=(m, chip_at(t) * 2 + core), device_id_type=MESH
        )
    pl.semaphore_signal(barrier, inc=1, device_id=(m, partner), device_id_type=MESH)

    def small(k):
        source, target = (
            (alpha_hbm, alpha), (root_hbm, root), (band_hbm, band), (gains_hbm, gains),
            (order_hbm, order_v), (order_hbm, order), (grad_hbm, grad),
        )[k]
        return pltpu.make_async_copy(source, target, small_sem.at[k])

    def load(r):
        q = chip_at(7 - r)
        return pltpu.make_async_copy(
            basis_hbm.at[pl.ds(pl.multiple_of(q * 256, 256), 256), :],
            basis.at[pl.ds(pl.multiple_of(r * 256, 256), 256), :],
            load_sem.at[r],
        )

    def load_anom(g):
        group = pl.ds(g * 4, 4)
        return pltpu.make_async_copy(anom_hbm.at[group], anom.at[group], asem.at[g])

    for k in range(7):
        small(k).start()
    for g in range(4):
        load_anom(g).start()
    load(0).start()
    load(1).start()
    for k in range(6):
        small(k).wait()

    bands = band[...]
    gain = jnp.zeros((1, 128), F32)
    for b in range(16):
        gain = jnp.where(bands == b, gains[0, b], gain)
    rooted = jnp.concatenate([root[...]] * 4, axis=0)
    rooted = jnp.concatenate([rooted] * 4, axis=1)
    row = lax.broadcasted_iota(jnp.int32, (128, 128), 0)
    col = lax.broadcasted_iota(jnp.int32, (128, 128), 1)
    rooted = jnp.where(row // 32 == col // 32, rooted, 0.0)

    def spread(halves, g, value):
        value = value.astype(BF16).reshape(4, 32, 128)
        for h in range(2):
            halves[h][pl.ds(z * 16 + g * 4, 4)] = value[:, h * 16:(h + 1) * 16, :]

    for g in range(4):
        rows = alpha[g * 4:(g + 1) * 4].astype(F32).reshape(128, 128)
        value = jnp.dot(rooted, rows, precision=HIGH, preferred_element_type=F32) * gain
        spread(zall, g, value)

    held = (order_v[...] == row).astype(F32).astype(BF16)
    slots = lax.broadcasted_iota(jnp.int32, (8, 128), 1).astype(F32).astype(BF16)
    inverse_v[...] = lax.dot_general(slots, held, NT, preferred_element_type=F32).astype(jnp.int32)
    to_scalars = pltpu.make_async_copy(inverse_v, inverse, small_sem.at[7])
    to_scalars.start()

    with scope("bar"):
        pl.semaphore_wait(barrier, 12)

    def z_copy(all_ref, h, dz, send, recv):
        mine = all_ref[h].at[pl.ds(z * 16, 16)]
        return remote(mine, mine, send.at[h], recv.at[h], ((z + dz) % 4) * 2 + yl, s)

    for dz in (2, 1, 3):
        z_copy(zall, 0, dz, z_s, z_r).start()
    to_scalars.wait()

    small(6).wait()
    for g in range(4):
        with scope("anomwait"):
            load_anom(g).wait()

        def weigh(c, carry):
            w = lanes(c * 512, 512)
            factor = grad[:, w].astype(F32)
            for k in range(4):
                value = (anom[g * 4 + k, :, w].astype(F32) * factor).astype(BF16)
                weighted[pl.ds(g * 128 + k * 32, 32), w] = value
            return carry

        lax.fori_loop(0, 8, weigh, 0)
        if g == 1:
            for dz in (2, 1, 3):
                z_copy(zall, 1, dz, z_s, z_r).start()

    def pick(table, all_ref, h, slot):
        where = jnp.bitwise_and(table[0, slot], 127)
        same = (where // 16) % 2 == yl
        return same, all_ref[h][(where // 32) * 16 + where % 16]

    def y_copy(src, dst, h, send, recv):
        levels = pl.ds(h * 16, 16)
        return remote(
            src.at[:, levels], dst.at[:, levels], send.at[h], recv.at[h], ymate, s
        )

    def exchange(table, all_ref, src, dst, h, zs, zr, ys, yr):
        wait_all(all_ref[h].at[pl.ds(0, 48)], zr.at[h])
        for i in range(16):
            same, value = pick(table, all_ref, h, ymate * 16 + i)
            src[i, pl.ds(h * 16, 16), :] = jnp.where(same, value, jnp.zeros_like(value))
        y_copy(src, dst, h, ys, yr).start()

    def piece(h, e, r, c):
        return coefs[h].at[pl.ds(e * 8, 8), :, lanes(r * 256 + c * 128, 128)]

    def b_copy(h, e, source, target, t, recv):
        return remote(
            piece(h, e, source, core), piece(h, e, target, core), b_s.at[0], recv.at[h],
            m, chip_at(t) * 2 + core,
        )

    def d_copy(h, e, r):
        here = piece(h, e, r, core)
        return remote(here, here, d_s.at[0], d_r.at[2 * h + r // 4], m, partner)

    def settle(h):
        y_copy(ysend, ypart, h, y_s, y_r).wait_recv()
        for i in range(16):
            same, value = pick(inverse, zall, h, m * 16 + i)
            coefs[h][i, :, lanes(7 * 256 + core * 128, 128)] = jnp.where(
                same, value, ypart[i, pl.ds(h * 16, 16), :]
            )

    def launch(h):
        b_copy(h, 0, 7, 3, 4, mate_r).start()
        for dx in (2, 1, 3):
            for e in range(2):
                b_copy(h, e, 7, 3 + dx, dx, row_r).start()
        b_copy(h, 1, 7, 3, 4, rest_r).start()
        for e in range(2):
            d_copy(h, e, 7).start()

    def relay_mate(h):
        wait_all(coefs[h].at[pl.ds(0, 8), :, pl.ds(0, 128)], mate_r.at[h])
        for dx in (2, 1, 3):
            b_copy(h, 0, 3, dx - 1, dx, rest_r).start()
        d_copy(h, 0, 3).start()

    def relay_row(h):
        wait_all(coefs[h].at[pl.ds(0, 3)], row_r.at[h])
        for dx in (1, 3, 2):
            b_copy(h, 1, 7 - dx, 3 - dx, 4, rest_r).start()
            for e in range(2):
                d_copy(h, e, 7 - dx).start()

    def relay_rest(h):
        wait_all(coefs[h].at[pl.ds(0, 7), :, pl.ds(0, 1024)], rest_r.at[h])
        for r in range(3):
            for e in range(2):
                d_copy(h, e, r).start()
        d_copy(h, 1, 3).start()

    def gathered(h, far):
        wait_all(coefs[h].at[pl.ds(0, 4)], d_r.at[2 * h + 1 - far])

    def x_copy(r):
        return remote(
            part.at[r, :, lanes(other * 128, 128)], half.at[r], x_s.at[0], x_r.at[r], m, partner
        )

    def r_copy(r):
        return remote(
            outgo.at[r], landed.at[r], r_s.at[0], r_r.at[r // 4], m,
            chip_at((7 - r) % 4) * 2 + core,
        )

    def ry_copy():
        return remote(rsend, rland, ry_s.at[0], ry_r.at[0], m, chip_at(4) * 2 + core)

    def own(r, rows):
        return part[r, rows, lanes(core * 128, 128)] + half[r, rows, :]

    def adjoint(r, carry):
        @pl.when(r < 6)
        def _():
            load(r + 2).start()

        with scope("bwait"):
            load(r).wait()
        rows = pl.ds(pl.multiple_of(r * 256, 256), 256)
        with scope("adot"):
            part[r] = lax.dot_general(weighted[...], basis[rows, :], NT, preferred_element_type=F32)
        x_copy(r).start()

        @pl.when(r > 0)
        def _():
            p = r - 1
            with scope("xwait"):
                x_copy(p).wait_recv()

            @pl.when(p != 3)
            def _():
                outgo[p] = (part[p, :, lanes(core * 128, 128)] + half[p]).astype(BF16)

            @pl.when(p < 3)
            def _():
                r_copy(p).start()

        @pl.when(r == 2)
        def _():
            with scope("z0wait"):
                exchange(inverse, zall, ysend, ypart, 0, z_s, z_r, y_s, y_r)

        @pl.when(r == 4)
        def _():
            with scope("z1wait"):
                exchange(inverse, zall, ysend, ypart, 1, z_s, z_r, y_s, y_r)
            with scope("y0wait"):
                settle(0)
            launch(0)

        @pl.when(r == 6)
        def _():
            with scope("y1wait"):
                settle(1)
            launch(1)

        return carry

    lax.fori_loop(0, 8, adjoint, 0)

    with scope("mate0wait"):
        relay_mate(0)
    with scope("row0wait"):
        relay_row(0)
    for r in range(4, 7):
        r_copy(r).start()

    with scope("rfwait"):
        wait_all(landed.at[pl.ds(0, 3)], r_r.at[0])
    for g in range(4):
        rows = pl.ds(g * 128, 128)
        total = own(3, rows)
        for r in range(3):
            total = total + landed[r, rows, :].astype(F32)
        rsend[rows, :] = total
    ry_copy().start()

    def i_copy(h, i):
        return remote(
            inc_send.at[h, i], inc_land.at[h, i], i_s.at[0], i_r.at[h], mem_at(7 - i), s
        )

    def o_copy(h, u):
        return remote(
            inc_own.at[h], inc_all.at[h, m], o_s.at[0], o_r.at[h], mem_at(u), s
        )

    def field(h, low, w):
        with scope("field"):
            f = jnp.dot(
                coefs[h][:, :, low:low + 1024].reshape(256, 1024), basis[low:low + 1024, w],
                preferred_element_type=F32,
            )
            levels = pl.ds(h * 16, 16)
            product = f.reshape(16, 16, 512) * anom[:, levels, w].astype(F32)
            return jnp.sum(product, axis=0)

    def near(h, i):
        w = lanes(i * 512, 512)
        inc_acc[h, :, w] = field(h, 1024, w)

    def far(h, i):
        w = lanes(mem_at(7 - i) * 512, 512)
        inc_send[h, i] = (field(h, 0, w) + inc_acc[h, :, w]).astype(BF16)

        @pl.when(i < 7)
        def _():
            i_copy(h, i).start()

    def reduce_own(h):
        total = inc_send[h, 7].astype(F32)
        wait_all(inc_land.at[h], i_r.at[h])
        for i in range(7):
            total = total + inc_land[h, i].astype(F32)
        inc_own[h] = total.astype(BF16)
        for u in (4, 5, 1, 2, 3, 6, 7):
            o_copy(h, u).start()

    def near0(i, carry):
        near(0, i)

        @pl.when(i == 3)
        def _():
            with scope("mate1wait"):
                relay_mate(1)

        @pl.when(i == 6)
        def _():
            with scope("rest0wait"):
                relay_rest(0)

        return carry

    def far0(i, carry):
        far(0, i)

        @pl.when(i == 1)
        def _():
            with scope("row1wait"):
                relay_row(1)

        return carry

    def near1(i, carry):
        near(1, i)

        @pl.when(i == 4)
        def _():
            with scope("rest1wait"):
                relay_rest(1)

        @pl.when(i == 1)
        def _():
            with scope("rnwait"):
                x_copy(7).wait_recv()
                wait_all(landed.at[pl.ds(4, 3)], r_r.at[1])
                ry_copy().wait_recv()
            for g in range(4):
                rows = pl.ds(g * 128, 128)
                total = own(7, rows) + rland[rows, :]
                for r in range(4, 7):
                    total = total + landed[r, rows, :].astype(F32)
                value = jnp.dot(rooted.T, total, precision=HIGH, preferred_element_type=F32) * gain
                spread(gall, g, value)
            for h in range(2):
                for dz in (2, 1, 3):
                    z_copy(gall, h, dz, gz_s, gz_r).start()

        return carry

    def far1(i, carry):
        far(1, i)

        @pl.when(i == 1)
        def _():
            with scope("i0wait"):
                reduce_own(0)

        @pl.when(i == 5)
        def _():
            with scope("gz0wait"):
                exchange(order, gall, gsend, gpart, 0, gz_s, gz_r, gy_s, gy_r)

        return carry

    with scope("dn0wait"):
        gathered(0, False)
    lax.fori_loop(0, 8, near0, 0)
    with scope("df0wait"):
        gathered(0, True)
    lax.fori_loop(0, 8, far0, 0)
    with scope("dn1wait"):
        gathered(1, False)
    lax.fori_loop(0, 8, near1, 0)
    with scope("df1wait"):
        gathered(1, True)
    lax.fori_loop(0, 8, far1, 0)

    with scope("i1wait"):
        reduce_own(1)
    with scope("gz1wait"):
        exchange(order, gall, gsend, gpart, 1, gz_s, gz_r, gy_s, gy_r)

    for h in range(2):
        with scope("gywait"):
            y_copy(gsend, gpart, h, gy_s, gy_r).wait_recv()
        for i in range(16):
            same, value = pick(order, gall, h, m * 16 + i)
            levels = pl.ds(h * 16, 16)
            ag_out[i, levels, :] = jnp.where(same, value, gpart[i, levels, :]).astype(F32)

    for h in range(2):
        levels = pl.ds(h * 16, 16)
        inc_out[levels, lanes(m * 512, 512)] = inc_own[h].astype(F32)
        with scope("owait"):
            wait_all(inc_all.at[h, pl.ds(0, 7)], o_r.at[h])
        for u in range(1, 8):
            spot = mem_at(u)
            inc_out[levels, lanes(spot * 512, 512)] = inc_all[h, spot].astype(F32)

    with scope("sentwait"):
        for h in range(2):
            wait_all(zall[h].at[pl.ds(0, 48)], z_s.at[h])
            wait_all(gall[h].at[pl.ds(0, 48)], gz_s.at[h])
            y_copy(ysend, ypart, h, y_s, y_r).wait_send()
            y_copy(gsend, gpart, h, gy_s, gy_r).wait_send()
        wait_all(coefs0.at[pl.ds(0, 14)], b_s.at[0])
        wait_all(coefs0, d_s.at[0])
        wait_all(inc_land, i_s.at[0])
        wait_all(inc_land, o_s.at[0])
        wait_all(outgo.at[pl.ds(0, 6)], r_s.at[0])
        wait_all(half, x_s.at[0])
        ry_copy().wait_send()


def on_device(anomalies, alpha, basis, gradient, vertical_root, band_gain, band, order):
    vmem = pl.BlockSpec(memory_space=pltpu.VMEM)
    hbm = pl.BlockSpec(memory_space=pl.ANY)
    dma = lambda n: pltpu.SemaphoreType.DMA((n,))
    int32 = jnp.int32
    return pl.pallas_call(
        kernel,
        out_shape=(
            pltpu.VMEM((32, 4096), F32),
            pltpu.VMEM((16, 32, 128), F32),
        ),
        in_specs=[hbm] * 8,
        out_specs=(vmem, vmem),
        scratch_shapes=[
            pltpu.VMEM((1, 128), int32),
            pltpu.SMEM((1, 128), int32),
            pltpu.VMEM((8, 128), int32),
            pltpu.SMEM((8, 128), int32),
            pltpu.SMEM((1, 16), F32),
            pltpu.VMEM((16, 32, 128), BF16),
            pltpu.VMEM((32, 4096), BF16),
            pltpu.VMEM((32, 32), F32),
            pltpu.VMEM((1, 128), int32),
            pltpu.VMEM((2048, 4096), BF16),
            pltpu.VMEM((16, 32, 4096), BF16),
            pltpu.VMEM((512, 4096), BF16),
            pltpu.VMEM((8, 512, 256), F32),
            pltpu.VMEM((8, 512, 128), F32),
            pltpu.VMEM((7, 512, 128), BF16),
            pltpu.VMEM((7, 512, 128), BF16),
            pltpu.VMEM((512, 128), F32),
            pltpu.VMEM((512, 128), F32),
            pltpu.VMEM((16, 16, 2048), BF16),
            pltpu.VMEM((16, 16, 2048), BF16),
            pltpu.VMEM((64, 16, 128), BF16),
            pltpu.VMEM((64, 16, 128), BF16),
            pltpu.VMEM((16, 32, 128), BF16),
            pltpu.VMEM((16, 32, 128), BF16),
            pltpu.VMEM((2, 16, 4096), F32),
            pltpu.VMEM((2, 8, 16, 512), BF16),
            pltpu.VMEM((2, 7, 16, 512), BF16),
            pltpu.VMEM((2, 16, 512), BF16),
            pltpu.VMEM((2, 8, 16, 512), BF16),
            pltpu.VMEM((64, 16, 128), BF16),
            pltpu.VMEM((64, 16, 128), BF16),
            pltpu.VMEM((16, 32, 128), BF16),
            pltpu.VMEM((16, 32, 128), BF16),
            dma(8), dma(8), dma(4), dma(2), dma(2), dma(2), dma(2), dma(1), dma(2), dma(2), dma(2),
            dma(1), dma(4), dma(1), dma(8), dma(1), dma(2), dma(1), dma(1), dma(1), dma(2),
            dma(1), dma(2), dma(2), dma(2), dma(2), dma(2),
        ],
        compiler_params=pltpu.CompilerParams(
            collective_id=0, has_side_effects=True, vmem_limit_bytes=60 << 20
        ),
    )(
        order.reshape(1, -1), band_gain.reshape(1, -1), anomalies, alpha, basis, gradient,
        vertical_root, band.reshape(1, -1),
    )


def solution(mesh):
    return jax.shard_map(
        on_device,
        mesh=mesh,
        in_specs=(
            P("mem", None, "state"),
            P("mem", None, "state"),
            P(None, "state"),
            P(None, "state"),
            P(),
            P(),
            P("state"),
            P(),
        ),
        out_specs=(P(None, "state"), P("mem", None, "state")),
        check_vma=False,
    )
```

```python
import jax
import jax.numpy as jnp
from jax import lax
from jax.experimental import pallas as pl
from jax.experimental.pallas import tpu as pltpu
from jax.sharding import PartitionSpec as P

MESH = pl.DeviceIdType.MESH
NT = (((1,), (1,)), ((), ()))
HIGH = lax.Precision.HIGHEST
F32 = jnp.float32
BF16 = jnp.bfloat16
scope = jax.named_scope


def kernel(
    order_hbm, gains_hbm, anom_hbm, alpha_hbm, basis_hbm, grad_hbm, root_hbm, band_hbm,
    inc_out, ag_out,
    order_v, order, inverse_v, inverse, gains, alpha, grad, root, band,
    basis, anom, weighted, part, half, outgo, relayed, landed, rsend, rland, coefs0, coefs1,
    zall, ypart, ysend, zpair, zout, zland, inc_acc, inc_send, inc_land, inc_own, inc_all, gall, gpart, gsend, gpair, gout, gland,
    small_sem, load_sem, asem, z_s, z_r, b_s, mate_r, row_r, rest_r, d_s, d_r, x_s, x_r,
    rd_s, rd_r, r_s, r_r, ry_s, ry_r, i_s, i_r, o_s, o_r, gz_s, gz_r,
):
    coefs = (coefs0, coefs1)
    m = lax.axis_index("mem")
    s = lax.axis_index("state")
    z, yl = m // 2, m % 2
    chip, core = s // 2, s % 2
    yh, x = chip // 4, chip % 4
    other = 1 - core

    def chip_at(t):
        return ((yh + t // 4) % 2) * 4 + (x + t % 4) % 4

    def mem_at(u):
        return ((z + u // 2) % 4) * 2 + (yl + u % 2) % 2

    def remote(src, dst, send, recv, mem, state):
        return pltpu.make_async_remote_copy(
            src_ref=src, dst_ref=dst, send_sem=send, recv_sem=recv,
            device_id=(mem, state), device_id_type=MESH,
        )

    def wait_all(ref, sem):
        pltpu.make_async_copy(ref, ref, sem).wait()

    def lanes(start, width):
        return pl.ds(pl.multiple_of(start, 128), width)

    partner = chip * 2 + other
    ymate = z * 2 + (1 - yl)

    barrier = pltpu.get_barrier_semaphore()
    for u in range(1, 8):
        pl.semaphore_signal(barrier, inc=1, device_id=(mem_at(u), s), device_id_type=MESH)
    for t in range(1, 5):
        pl.semaphore_signal(
            barrier, inc=1, device_id=(m, chip_at(t) * 2 + core), device_id_type=MESH
        )
    pl.semaphore_signal(barrier, inc=1, device_id=(m, partner), device_id_type=MESH)

    def small(k):
        source, target = (
            (alpha_hbm, alpha), (root_hbm, root), (band_hbm, band), (gains_hbm, gains),
            (order_hbm, order_v), (order_hbm, order), (grad_hbm, grad),
        )[k]
        return pltpu.make_async_copy(source, target, small_sem.at[k])

    def slot_at(r):
        a, b = (r % 4) // 2, r % 2
        return (r // 4) * 4 + 3 - (2 + a - b * (1 + 2 * a))

    def load(r):
        slot = slot_at(r)
        q = chip_at(7 - slot)
        return pltpu.make_async_copy(
            basis_hbm.at[pl.ds(pl.multiple_of(q * 256, 256), 256), :],
            basis.at[pl.ds(pl.multiple_of(slot * 256, 256), 256), :],
            load_sem.at[r],
        )

    def load_anom(g):
        group = pl.ds(g * 4, 4)
        return pltpu.make_async_copy(anom_hbm.at[group], anom.at[group], asem.at[g])

    for k in range(7):
        small(k).start()
    for g in range(4):
        load_anom(g).start()
    load(0).start()
    with scope("smallwait"):
        for k in range(6):
            small(k).wait()

    bands = band[...]
    gain = jnp.zeros((1, 128), F32)
    for b in range(16):
        gain = jnp.where(bands == b, gains[0, b], gain)
    rooted = jnp.concatenate([root[...]] * 4, axis=0)
    rooted = jnp.concatenate([rooted] * 4, axis=1)
    row = lax.broadcasted_iota(jnp.int32, (128, 128), 0)
    col = lax.broadcasted_iota(jnp.int32, (128, 128), 1)
    rooted = jnp.where(row // 32 == col // 32, rooted, 0.0)

    def spread(all_ref, pair, g, value):
        value = value.astype(BF16).reshape(4, 32, 128)
        all_ref[pl.ds(z * 16 + g * 4, 4)] = value[:, :16, :]
        pair[pl.ds(yl * 16 + g * 4, 4)] = value[:, 16:, :]

    for g in range(4):
        rows = alpha[g * 4:(g + 1) * 4].astype(F32).reshape(128, 128)
        value = jnp.dot(rooted, rows, precision=HIGH, preferred_element_type=F32) * gain
        spread(zall, zpair, g, value)

    held = (order_v[...] == row).astype(F32).astype(BF16)
    slots = lax.broadcasted_iota(jnp.int32, (8, 128), 1).astype(F32).astype(BF16)
    inverse_v[...] = lax.dot_general(slots, held, NT, preferred_element_type=F32).astype(jnp.int32)
    to_scalars = pltpu.make_async_copy(inverse_v, inverse, small_sem.at[7])
    to_scalars.start()

    with scope("bar"):
        pl.semaphore_wait(barrier, 12)

    def z_copy(all_ref, dz, send, recv):
        mine = all_ref.at[pl.ds(z * 16, 16)]
        return remote(mine, mine, send.at[0], recv.at[0], ((z + dz) % 4) * 2 + yl, s)

    def y_copy(src, dst, send, recv):
        return remote(src, dst, send.at[1], recv.at[1], ymate, s)

    def pair_copy(pair, send, recv):
        mine = pair.at[pl.ds(yl * 16, 16)]
        return remote(mine, mine, send.at[2], recv.at[2], ymate, s)

    def out_copy(out, land, dz, send, recv):
        return remote(
            out.at[dz - 1], land.at[pl.ds(z * 16, 16)], send.at[3], recv.at[3],
            ((z + dz) % 4) * 2 + yl, s,
        )

    def depart(all_ref, pair, send, recv):
        for dz in (2, 1, 3):
            z_copy(all_ref, dz, send, recv).start()
        pair_copy(pair, send, recv).start()

    depart(zall, zpair, z_s, z_r)
    to_scalars.wait()

    small(6).wait()
    for g in range(4):
        with scope("anomwait"):
            load_anom(g).wait()
        if g == 1:
            load(1).start()

        def weigh(c, carry):
            w = lanes(c * 512, 512)
            factor = grad[:, w].astype(F32)
            for k in range(4):
                value = (anom[g * 4 + k, :, w].astype(F32) * factor).astype(BF16)
                weighted[pl.ds(g * 128 + k * 32, 32), w] = value
            return carry

        lax.fori_loop(0, 8, weigh, 0)

    def held_at(table, slot):
        return jnp.bitwise_and(table[0, slot], 127)

    def gathered_row(all_ref, where):
        return all_ref[(where // 32) * 16 + where % 16]

    def to_mate(table, all_ref, src, dst, send, recv):
        wait_all(all_ref.at[pl.ds(0, 48)], recv.at[0])
        for i in range(16):
            src[i] = gathered_row(all_ref, held_at(table, ymate * 16 + i))
        y_copy(src, dst, send, recv).start()

    def to_z(table, pair, out, land, send, recv):
        pair_copy(pair, send, recv).wait_recv()
        for dz in (2, 1, 3):
            for i in range(16):
                where = held_at(table, (((z + dz) % 4) * 2 + yl) * 16 + i)
                out[dz - 1, i] = pair[where % 32]
            out_copy(out, land, dz, send, recv).start()
        for i in range(16):
            land[z * 16 + i] = pair[held_at(table, m * 16 + i) % 32]

    def arrived(table, h, all_ref, src, dst, land, send, recv):
        if h:
            wait_all(land.at[pl.ds(0, 48)], recv.at[3])
        else:
            y_copy(src, dst, send, recv).wait_recv()
        for i in range(16):
            where = held_at(table, m * 16 + i)
            if h:
                yield i, land[(where // 32) * 16 + i]
            else:
                same = (where // 16) % 2 == yl
                yield i, jnp.where(same, gathered_row(all_ref, where), dst[i])

    def parts(h):
        return (0, 1) if h == 0 else (0,)

    def piece(h, e, r, c):
        count = 16 // len(parts(h))
        return coefs[h].at[pl.ds(e * count, count), :, lanes(r * 256 + c * 128, 128)]

    def b_copy(h, e, source, target, t, recv):
        return remote(
            piece(h, e, source, core), piece(h, e, target, core), b_s.at[0], recv.at[h],
            m, chip_at(t) * 2 + core,
        )

    def d_copy(h, e, r):
        here = piece(h, e, r, core)
        return remote(here, here, d_s.at[0], d_r.at[2 * h + r // 4], m, partner)

    def settle(h):
        for i, value in arrived(inverse, h, zall, ysend, ypart, zland, z_s, z_r):
            coefs[h][i, :, lanes(7 * 256 + core * 128, 128)] = value

    def launch_y(h):
        b_copy(h, 0, 7, 3, 4, mate_r).start()
        if h == 0:
            b_copy(h, 1, 7, 3, 4, rest_r).start()
        for e in parts(h):
            d_copy(h, e, 7).start()

    def launch_x(h):
        for dx in (2, 1, 3):
            for e in parts(h):
                b_copy(h, e, 7, 3 + dx, dx, row_r).start()

    def relay_mate(h):
        wait_all(piece(h, 0, 3, core), mate_r.at[h])
        for dx in (2, 1, 3):
            b_copy(h, 0, 3, dx - 1, dx, rest_r).start()
        d_copy(h, 0, 3).start()

    def relay_row(h):
        wait_all(coefs[h].at[pl.ds(0, 3)], row_r.at[h])
        for dx in (1, 3, 2):
            if h == 0:
                b_copy(h, 1, 7 - dx, 3 - dx, 4, rest_r).start()
            for e in parts(h):
                d_copy(h, e, 7 - dx).start()

    def relay_rest(h):
        if h == 0:
            wait_all(coefs[h].at[pl.ds(0, 7), :, pl.ds(0, 1024)], rest_r.at[h])
            d_copy(h, 1, 3).start()
        else:
            wait_all(coefs[h].at[pl.ds(0, 3)], rest_r.at[h])
        for r in range(3):
            for e in parts(h):
                d_copy(h, e, r).start()

    def gathered(h, far):
        wait_all(coefs[h].at[pl.ds(0, 4)], d_r.at[2 * h + 1 - far])

    def x_copy(r):
        return remote(
            part.at[r, :, lanes(other * 128, 128)], half.at[r], x_s.at[0], x_r.at[r], m, partner
        )

    def rd_copy(g, side):
        rows = pl.ds(side * 256, 256)
        return remote(
            outgo.at[4 * g + 1, rows], relayed.at[g, rows], rd_s.at[0], rd_r.at[g], m,
            chip_at(1 + 2 * side) * 2 + core,
        )

    def r_copy(g, side):
        slot = 4 * g + 2 - 2 * side
        return remote(
            outgo.at[slot], landed.at[g, side], r_s.at[0], r_r.at[g], m,
            chip_at(1 + 2 * side) * 2 + core,
        )

    def pass_half(g):
        slot = 4 * g + 1
        outgo[slot] = own(slot, pl.ds(0, 512)).astype(BF16)
        for side in range(2):
            rd_copy(g, side).start()

    def combine(g):
        wait_all(relayed.at[g], rd_r.at[g])
        for side in range(2):
            slot = 4 * g + 2 - 2 * side
            for part_side in range(2):
                rows = pl.ds(part_side * 256, 256)
                total = own(slot, rows)
                if part_side == side:
                    total = total + relayed[g, rows, :].astype(F32)
                outgo[slot, rows, :] = total.astype(BF16)
            r_copy(g, side).start()

    def summed(g, rows):
        total = own(4 * g + 3, rows)
        for side in range(2):
            total = total + landed[g, side, rows, :].astype(F32)
        return total

    def ry_copy():
        return remote(rsend, rland, ry_s.at[0], ry_r.at[0], m, chip_at(4) * 2 + core)

    def own(r, rows):
        return part[r, rows, lanes(core * 128, 128)] + half[r, rows, :]

    def adjoint(r, carry):
        @pl.when(r < 6)
        def _():
            load(r + 2).start()

        with scope("bwait"):
            load(r).wait()
        slot = slot_at(r)
        rows = pl.ds(pl.multiple_of(slot * 256, 256), 256)
        with scope("adot"):
            part[slot] = lax.dot_general(
                weighted[...], basis[rows, :], NT, preferred_element_type=F32
            )
        x_copy(slot).start()

        @pl.when(r > 0)
        def _():
            with scope("xwait"):
                x_copy(slot_at(r - 1)).wait_recv()

        @pl.when(r == 0)
        def _():
            with scope("p1wait"):
                to_z(inverse, zpair, zout, zland, z_s, z_r)

        @pl.when(r == 1)
        def _():
            pass_half(0)
            with scope("z0wait"):
                to_mate(inverse, zall, ysend, ypart, z_s, z_r)

        @pl.when(r == 3)
        def _():
            with scope("s0wait"):
                settle(0)
            launch_y(0)
            launch_x(0)
            with scope("c0wait"):
                combine(0)

        @pl.when(r == 4)
        def _():
            with scope("s1wait"):
                settle(1)
            launch_y(1)

        @pl.when(r == 5)
        def _():
            with scope("mate0wait"):
                relay_mate(0)
            launch_x(1)
            pass_half(1)

        @pl.when(r == 6)
        def _():
            with scope("row0wait"):
                relay_row(0)

        return carry

    lax.fori_loop(0, 8, adjoint, 0)
    with scope("mate1wait"):
        relay_mate(1)

    def i_copy(h, i, y):
        return remote(
            inc_send.at[h, i, y], inc_land.at[h, 2 * i + yl], i_s.at[0], i_r.at[h],
            ((z + 3 - i) % 4) * 2 + y, s,
        )

    def o_copy(h, u):
        return remote(
            inc_own.at[h], inc_all.at[h, m], o_s.at[0], o_r.at[h], mem_at(u), s
        )

    def field(h, low, w):
        with scope("field"):
            f = jnp.dot(
                coefs[h][:, :, low:low + 1024].reshape(256, 1024), basis[low:low + 1024, w],
                preferred_element_type=F32,
            )
            levels = pl.ds(h * 16, 16)
            product = f.reshape(16, 16, 1024) * anom[:, levels, w].astype(F32)
            return jnp.sum(product, axis=0)

    def near(h, i):
        w = lanes(i * 1024, 1024)
        inc_acc[h, :, w] = field(h, 1024, w)

    def far(h, i):
        w = lanes(((z + 3 - i) % 4) * 1024, 1024)
        value = (field(h, 0, w) + inc_acc[h, :, w]).astype(BF16)
        for y in range(2):
            inc_send[h, i, y] = value[:, y * 512:(y + 1) * 512]

        @pl.when(i < 3)
        def _():
            for y in range(2):
                i_copy(h, i, y).start()

        @pl.when(i == 3)
        def _():
            i_copy(h, i, 1 - yl).start()

    def reduce_own(h):
        total = inc_send[h, 3, yl].astype(F32)
        wait_all(inc_land.at[h, pl.ds(0, 7)], i_r.at[h])
        for k in range(6):
            total = total + inc_land[h, k].astype(F32)
        total = total + inc_land[h, 7 - yl].astype(F32)
        inc_own[h] = total.astype(BF16)
        for u in (5, 4, 3, 7, 1, 2, 6):
            o_copy(h, u).start()

    def near0(i, carry):
        near(0, i)

        @pl.when(i == 1)
        def _():
            with scope("rfwait"):
                wait_all(landed.at[0], r_r.at[0])
            for g in range(4):
                rows = pl.ds(g * 128, 128)
                rsend[rows, :] = summed(0, rows)
            ry_copy().start()

        @pl.when(i == 3)
        def _():
            with scope("rest0wait"):
                relay_rest(0)

        return carry

    def far0(i, carry):
        far(0, i)

        @pl.when(i == 1)
        def _():
            with scope("row1wait"):
                relay_row(1)
            with scope("c1wait"):
                combine(1)

        return carry

    def near1(i, carry):
        near(1, i)

        @pl.when(i == 2)
        def _():
            with scope("rest1wait"):
                relay_rest(1)

        return carry

    def far1(i, carry):
        far(1, i)

        @pl.when(i == 1)
        def _():
            with scope("i0wait"):
                reduce_own(0)

        return carry

    with scope("dn0wait"):
        gathered(0, False)
    lax.fori_loop(0, 4, near0, 0)
    with scope("df0wait"):
        gathered(0, True)
    lax.fori_loop(0, 4, far0, 0)
    with scope("dn1wait"):
        gathered(1, False)
    lax.fori_loop(0, 4, near1, 0)
    with scope("rnwait"):
        x_copy(7).wait_recv()
        wait_all(landed.at[1], r_r.at[1])
        ry_copy().wait_recv()
    for g in range(4):
        rows = pl.ds(g * 128, 128)
        total = summed(1, rows) + rland[rows, :]
        value = jnp.dot(rooted.T, total, precision=HIGH, preferred_element_type=F32) * gain
        spread(gall, gpair, g, value)
    depart(gall, gpair, gz_s, gz_r)
    with scope("df1wait"):
        gathered(1, True)
    lax.fori_loop(0, 4, far1, 0)

    with scope("gp1wait"):
        to_z(order, gpair, gout, gland, gz_s, gz_r)
    with scope("gz0wait"):
        to_mate(order, gall, gsend, gpart, gz_s, gz_r)
    with scope("i1wait"):
        reduce_own(1)
    for h in (1, 0):
        with scope("gs%dwait" % h):
            for i, value in arrived(order, h, gall, gsend, gpart, gland, gz_s, gz_r):
                ag_out[i, pl.ds(h * 16, 16), :] = value.astype(F32)

    for h in range(2):
        levels = pl.ds(h * 16, 16)
        inc_out[levels, lanes(m * 512, 512)] = inc_own[h].astype(F32)
        with scope("owait"):
            wait_all(inc_all.at[h, pl.ds(0, 7)], o_r.at[h])
        for u in range(1, 8):
            spot = mem_at(u)
            inc_out[levels, lanes(spot * 512, 512)] = inc_all[h, spot].astype(F32)

    with scope("sentwait"):
        for all_ref, src, dst, pair, send, recv in (
            (zall, ysend, ypart, zpair, z_s, z_r), (gall, gsend, gpart, gpair, gz_s, gz_r)
        ):
            wait_all(all_ref.at[pl.ds(0, 48)], send.at[0])
            y_copy(src, dst, send, recv).wait_send()
            pair_copy(pair, send, recv).wait_send()
            wait_all(all_ref.at[pl.ds(0, 48)], send.at[3])
        wait_all(coefs0.at[pl.ds(0, 14)], b_s.at[0])
        wait_all(coefs0, d_s.at[0])
        wait_all(inc_land.at[:, pl.ds(0, 7)], i_s.at[0])
        wait_all(inc_land.at[:, pl.ds(0, 7)], o_s.at[0])
        wait_all(relayed, rd_s.at[0])
        wait_all(landed, r_s.at[0])
        wait_all(half, x_s.at[0])
        ry_copy().wait_send()


def on_device(anomalies, alpha, basis, gradient, vertical_root, band_gain, band, order):
    vmem = pl.BlockSpec(memory_space=pltpu.VMEM)
    hbm = pl.BlockSpec(memory_space=pl.ANY)
    dma = lambda n: pltpu.SemaphoreType.DMA((n,))
    int32 = jnp.int32
    return pl.pallas_call(
        kernel,
        out_shape=(
            pltpu.VMEM((32, 4096), F32),
            pltpu.VMEM((16, 32, 128), F32),
        ),
        in_specs=[hbm] * 8,
        out_specs=(vmem, vmem),
        scratch_shapes=[
            pltpu.VMEM((1, 128), int32),
            pltpu.SMEM((1, 128), int32),
            pltpu.VMEM((8, 128), int32),
            pltpu.SMEM((8, 128), int32),
            pltpu.SMEM((1, 16), F32),
            pltpu.VMEM((16, 32, 128), BF16),
            pltpu.VMEM((32, 4096), BF16),
            pltpu.VMEM((32, 32), F32),
            pltpu.VMEM((1, 128), int32),
            pltpu.VMEM((2048, 4096), BF16),
            pltpu.VMEM((16, 32, 4096), BF16),
            pltpu.VMEM((512, 4096), BF16),
            pltpu.VMEM((8, 512, 256), F32),
            pltpu.VMEM((8, 512, 128), F32),
            pltpu.VMEM((7, 512, 128), BF16),
            pltpu.VMEM((2, 512, 128), BF16),
            pltpu.VMEM((2, 2, 512, 128), BF16),
            pltpu.VMEM((512, 128), F32),
            pltpu.VMEM((512, 128), F32),
            pltpu.VMEM((16, 16, 2048), BF16),
            pltpu.VMEM((16, 16, 2048), BF16),
            pltpu.VMEM((64, 16, 128), BF16),
            pltpu.VMEM((16, 16, 128), BF16),
            pltpu.VMEM((16, 16, 128), BF16),
            pltpu.VMEM((32, 16, 128), BF16),
            pltpu.VMEM((3, 16, 16, 128), BF16),
            pltpu.VMEM((64, 16, 128), BF16),
            pltpu.VMEM((2, 16, 4096), F32),
            pltpu.VMEM((2, 4, 2, 16, 512), BF16),
            pltpu.VMEM((2, 8, 16, 512), BF16),
            pltpu.VMEM((2, 16, 512), BF16),
            pltpu.VMEM((2, 8, 16, 512), BF16),
            pltpu.VMEM((64, 16, 128), BF16),
            pltpu.VMEM((16, 16, 128), BF16),
            pltpu.VMEM((16, 16, 128), BF16),
            pltpu.VMEM((32, 16, 128), BF16),
            pltpu.VMEM((3, 16, 16, 128), BF16),
            pltpu.VMEM((64, 16, 128), BF16),
            dma(8), dma(8), dma(4), dma(4), dma(4), dma(1), dma(2), dma(2), dma(2),
            dma(1), dma(4), dma(1), dma(8), dma(1), dma(2), dma(1), dma(2), dma(1), dma(1), dma(1),
            dma(2), dma(1), dma(2), dma(4), dma(4),
        ],
        compiler_params=pltpu.CompilerParams(
            collective_id=0, has_side_effects=True, vmem_limit_bytes=60 << 20
        ),
    )(
        order.reshape(1, -1), band_gain.reshape(1, -1), anomalies, alpha, basis, gradient,
        vertical_root, band.reshape(1, -1),
    )


def solution(mesh):
    return jax.shard_map(
        on_device,
        mesh=mesh,
        in_specs=(
            P("mem", None, "state"),
            P("mem", None, "state"),
            P(None, "state"),
            P(None, "state"),
            P(),
            P(),
            P("state"),
            P(),
        ),
        out_specs=(P(None, "state"), P("mem", None, "state")),
        check_vma=False,
    )
```

```python
import jax
import jax.numpy as jnp
from jax import lax
from jax.experimental import pallas as pl
from jax.experimental.pallas import tpu as pltpu
from jax.sharding import PartitionSpec as P

MESH = pl.DeviceIdType.MESH
NT = (((1,), (1,)), ((), ()))
HIGH = lax.Precision.HIGHEST
F32 = jnp.float32
BF16 = jnp.bfloat16
scope = jax.named_scope


def kernel(
    order_hbm, gains_hbm, anom_hbm, alpha_hbm, basis_hbm, grad_hbm, root_hbm, band_hbm,
    inc_out, ag_out,
    order_v, order, inverse_v, inverse, gains, alpha, grad, root, band,
    basis, anom, weighted, part, half, outgo, relayed, landed, rsend, rland, coefs0, coefs1,
    zall, ypart, ysend, zpair, zout, zland, inc_acc, inc_send, inc_land, inc_own, inc_all, gall, gpart, gsend, gpair, gout, gland,
    small_sem, load_sem, asem, z_s, z_r, b_s, mate_r, row_r, rest_r, d_s, d_r, x_s, x_r,
    rd_s, rd_r, r_s, r_r, ry_s, ry_r, i_s, i_r, o_s, o_r, gz_s, gz_r,
):
    coefs = (coefs0, coefs1)
    m = lax.axis_index("mem")
    s = lax.axis_index("state")
    z, yl = m // 2, m % 2
    chip, core = s // 2, s % 2
    yh, x = chip // 4, chip % 4
    other = 1 - core

    def chip_at(t):
        return ((yh + t // 4) % 2) * 4 + (x + t % 4) % 4

    def mem_at(u):
        return ((z + u // 2) % 4) * 2 + (yl + u % 2) % 2

    def remote(src, dst, send, recv, mem, state):
        return pltpu.make_async_remote_copy(
            src_ref=src, dst_ref=dst, send_sem=send, recv_sem=recv,
            device_id=(mem, state), device_id_type=MESH,
        )

    def wait_all(ref, sem):
        pltpu.make_async_copy(ref, ref, sem).wait()

    def lanes(start, width):
        return pl.ds(pl.multiple_of(start, 128), width)

    partner = chip * 2 + other
    ymate = z * 2 + (1 - yl)

    barrier = pltpu.get_barrier_semaphore()
    for u in range(1, 8):
        pl.semaphore_signal(barrier, inc=1, device_id=(mem_at(u), s), device_id_type=MESH)
    for t in range(1, 5):
        pl.semaphore_signal(
            barrier, inc=1, device_id=(m, chip_at(t) * 2 + core), device_id_type=MESH
        )
    pl.semaphore_signal(barrier, inc=1, device_id=(m, partner), device_id_type=MESH)

    def small(k):
        source, target = (
            (alpha_hbm, alpha), (root_hbm, root), (band_hbm, band), (gains_hbm, gains),
            (order_hbm, order_v), (order_hbm, order), (grad_hbm, grad),
        )[k]
        return pltpu.make_async_copy(source, target, small_sem.at[k])

    def slot_at(r):
        a, b = (r % 4) // 2, r % 2
        return (r // 4) * 4 + 3 - (2 + a - b * (1 + 2 * a))

    def load(r):
        slot = slot_at(r)
        q = chip_at(7 - slot)
        return pltpu.make_async_copy(
            basis_hbm.at[pl.ds(pl.multiple_of(q * 256, 256), 256), :],
            basis.at[pl.ds(pl.multiple_of(slot * 256, 256), 256), :],
            load_sem.at[r],
        )

    def load_anom(g):
        group = pl.ds(g * 4, 4)
        return pltpu.make_async_copy(anom_hbm.at[group], anom.at[group], asem.at[g])

    for k in range(7):
        small(k).start()
    for g in range(4):
        load_anom(g).start()
    load(0).start()
    with scope("smallwait"):
        for k in range(6):
            small(k).wait()

    bands = band[...]
    gain = jnp.zeros((1, 128), F32)
    for b in range(16):
        gain = jnp.where(bands == b, gains[0, b], gain)
    rooted = jnp.concatenate([root[...]] * 4, axis=0)
    rooted = jnp.concatenate([rooted] * 4, axis=1)
    row = lax.broadcasted_iota(jnp.int32, (128, 128), 0)
    col = lax.broadcasted_iota(jnp.int32, (128, 128), 1)
    rooted = jnp.where(row // 32 == col // 32, rooted, 0.0)

    def spread(all_ref, pair, g, value):
        value = value.astype(BF16).reshape(4, 32, 128)
        all_ref[pl.ds(z * 16 + g * 4, 4)] = value[:, :16, :]
        pair[pl.ds(yl * 16 + g * 4, 4)] = value[:, 16:, :]

    for g in range(4):
        rows = alpha[g * 4:(g + 1) * 4].astype(F32).reshape(128, 128)
        value = jnp.dot(rooted, rows, precision=HIGH, preferred_element_type=F32) * gain
        spread(zall, zpair, g, value)

    held = (order_v[...] == row).astype(F32).astype(BF16)
    slots = lax.broadcasted_iota(jnp.int32, (8, 128), 1).astype(F32).astype(BF16)
    inverse_v[...] = lax.dot_general(slots, held, NT, preferred_element_type=F32).astype(jnp.int32)
    to_scalars = pltpu.make_async_copy(inverse_v, inverse, small_sem.at[7])
    to_scalars.start()

    with scope("bar"):
        pl.semaphore_wait(barrier, 12)

    def z_copy(all_ref, dz, send, recv):
        mine = all_ref.at[pl.ds(z * 16, 16)]
        return remote(mine, mine, send.at[0], recv.at[0], ((z + dz) % 4) * 2 + yl, s)

    def y_copy(src, dst, send, recv):
        return remote(src, dst, send.at[1], recv.at[1], ymate, s)

    def pair_copy(pair, send, recv):
        mine = pair.at[pl.ds(yl * 16, 16)]
        return remote(mine, mine, send.at[2], recv.at[2], ymate, s)

    def out_copy(out, land, dz, send, recv):
        return remote(
            out.at[dz - 1], land.at[pl.ds(z * 16, 16)], send.at[3], recv.at[3],
            ((z + dz) % 4) * 2 + yl, s,
        )

    def depart(all_ref, pair, send, recv):
        for dz in (2, 1, 3):
            z_copy(all_ref, dz, send, recv).start()
        pair_copy(pair, send, recv).start()

    depart(zall, zpair, z_s, z_r)
    to_scalars.wait()

    small(6).wait()
    for g in range(4):
        with scope("anomwait"):
            load_anom(g).wait()
        if g == 1:
            load(1).start()

        def weigh(c, carry):
            w = lanes(c * 512, 512)
            factor = grad[:, w].astype(F32)
            for k in range(4):
                value = (anom[g * 4 + k, :, w].astype(F32) * factor).astype(BF16)
                weighted[pl.ds(g * 128 + k * 32, 32), w] = value
            return carry

        lax.fori_loop(0, 8, weigh, 0)

    def held_at(table, slot):
        return jnp.bitwise_and(table[0, slot], 127)

    def gathered_row(all_ref, where):
        return all_ref[(where // 32) * 16 + where % 16]

    def to_mate(table, all_ref, src, dst, send, recv):
        wait_all(all_ref.at[pl.ds(0, 48)], recv.at[0])
        for i in range(16):
            src[i] = gathered_row(all_ref, held_at(table, ymate * 16 + i))
        y_copy(src, dst, send, recv).start()

    def to_z(table, pair, out, land, send, recv):
        pair_copy(pair, send, recv).wait_recv()
        for dz in (2, 1, 3):
            for i in range(16):
                where = held_at(table, (((z + dz) % 4) * 2 + yl) * 16 + i)
                out[dz - 1, i] = pair[where % 32]
            out_copy(out, land, dz, send, recv).start()
        for i in range(16):
            land[z * 16 + i] = pair[held_at(table, m * 16 + i) % 32]

    def arrived(table, h, all_ref, src, dst, land, send, recv):
        if h:
            wait_all(land.at[pl.ds(0, 48)], recv.at[3])
        else:
            y_copy(src, dst, send, recv).wait_recv()
        for i in range(16):
            where = held_at(table, m * 16 + i)
            if h:
                yield i, land[(where // 32) * 16 + i]
            else:
                same = (where // 16) % 2 == yl
                yield i, jnp.where(same, gathered_row(all_ref, where), dst[i])

    def parts(h):
        return (0, 1) if h == 0 else (0,)

    def piece(h, e, r, c):
        count = 16 // len(parts(h))
        return coefs[h].at[pl.ds(e * count, count), :, lanes(r * 256 + c * 128, 128)]

    def b_copy(h, e, source, target, t, recv):
        return remote(
            piece(h, e, source, core), piece(h, e, target, core), b_s.at[0], recv.at[h],
            m, chip_at(t) * 2 + core,
        )

    def d_copy(h, e, r):
        here = piece(h, e, r, core)
        return remote(here, here, d_s.at[0], d_r.at[2 * h + r // 4], m, partner)

    def settle(h):
        for i, value in arrived(inverse, h, zall, ysend, ypart, zland, z_s, z_r):
            coefs[h][i, :, lanes(7 * 256 + core * 128, 128)] = value

    def launch_y(h):
        b_copy(h, 0, 7, 3, 4, mate_r).start()
        if h == 0:
            b_copy(h, 1, 7, 3, 4, rest_r).start()
        for e in parts(h):
            d_copy(h, e, 7).start()

    def launch_x(h):
        for dx in (2, 1, 3):
            for e in parts(h):
                b_copy(h, e, 7, 3 + dx, dx, row_r).start()

    def relay_mate(h):
        wait_all(piece(h, 0, 3, core), mate_r.at[h])
        for dx in (2, 1, 3):
            b_copy(h, 0, 3, dx - 1, dx, rest_r).start()
        d_copy(h, 0, 3).start()

    def relay_row(h):
        wait_all(coefs[h].at[pl.ds(0, 3)], row_r.at[h])
        for dx in (1, 3, 2):
            if h == 0:
                b_copy(h, 1, 7 - dx, 3 - dx, 4, rest_r).start()
            for e in parts(h):
                d_copy(h, e, 7 - dx).start()

    def relay_rest(h):
        if h == 0:
            wait_all(coefs[h].at[pl.ds(0, 7), :, pl.ds(0, 1024)], rest_r.at[h])
            d_copy(h, 1, 3).start()
        else:
            wait_all(coefs[h].at[pl.ds(0, 3)], rest_r.at[h])
        for r in range(3):
            for e in parts(h):
                d_copy(h, e, r).start()

    def gathered(h, far):
        wait_all(coefs[h].at[pl.ds(0, 4)], d_r.at[2 * h + 1 - far])

    def x_copy(r):
        return remote(
            part.at[r, :, lanes(other * 128, 128)], half.at[r], x_s.at[0], x_r.at[r], m, partner
        )

    def came(slot):
        x_copy(slot).wait_recv()

    def rd_copy(g, side):
        rows = pl.ds(side * 256, 256)
        return remote(
            outgo.at[4 * g + 1, rows], relayed.at[g, rows], rd_s.at[0], rd_r.at[g], m,
            chip_at(1 + 2 * side) * 2 + core,
        )

    def r_copy(g, side):
        slot = 4 * g + 2 - 2 * side
        return remote(
            outgo.at[slot], landed.at[g, side], r_s.at[0], r_r.at[g], m,
            chip_at(1 + 2 * side) * 2 + core,
        )

    def pass_half(g):
        slot = 4 * g + 1
        outgo[slot] = own(slot, pl.ds(0, 512)).astype(BF16)
        for side in range(2):
            rd_copy(g, side).start()

    def combine(g):
        wait_all(relayed.at[g], rd_r.at[g])
        for side in range(2):
            slot = 4 * g + 2 - 2 * side
            for part_side in range(2):
                rows = pl.ds(part_side * 256, 256)
                total = own(slot, rows)
                if part_side == side:
                    total = total + relayed[g, rows, :].astype(F32)
                outgo[slot, rows, :] = total.astype(BF16)
            r_copy(g, side).start()

    def summed(g, rows):
        total = own(4 * g + 3, rows)
        for side in range(2):
            total = total + landed[g, side, rows, :].astype(F32)
        return total

    def ry_copy():
        return remote(rsend, rland, ry_s.at[0], ry_r.at[0], m, chip_at(4) * 2 + core)

    def own(r, rows):
        return part[r, rows, lanes(core * 128, 128)] + half[r, rows, :]

    def adjoint(r, carry):
        @pl.when(r < 6)
        def _():
            load(r + 2).start()

        with scope("bwait"):
            load(r).wait()
        slot = slot_at(r)
        rows = pl.ds(pl.multiple_of(slot * 256, 256), 256)
        with scope("adot"):
            part[slot] = lax.dot_general(
                weighted[...], basis[rows, :], NT, preferred_element_type=F32
            )
        x_copy(slot).start()

        @pl.when(r == 1)
        def _():
            with scope("z0wait"):
                to_mate(inverse, zall, ysend, ypart, z_s, z_r)
            with scope("xwait"):
                came(slot_at(0))
            pass_half(0)
            with scope("p1wait"):
                to_z(inverse, zpair, zout, zland, z_s, z_r)

        @pl.when(r == 3)
        def _():
            with scope("s0wait"):
                settle(0)
            launch_y(0)
            launch_x(0)
            with scope("c0wait"):
                came(slot_at(1))
                came(slot_at(2))
                combine(0)

        @pl.when(r == 4)
        def _():
            with scope("s1wait"):
                settle(1)
            launch_y(1)

        @pl.when(r == 5)
        def _():
            with scope("mate0wait"):
                relay_mate(0)
            launch_x(1)
            with scope("xwait"):
                came(slot_at(4))
            pass_half(1)

        @pl.when(r == 6)
        def _():
            with scope("row0wait"):
                relay_row(0)

        return carry

    lax.fori_loop(0, 8, adjoint, 0)
    with scope("mate1wait"):
        relay_mate(1)

    def i_copy(h, i, y):
        return remote(
            inc_send.at[h, i, y], inc_land.at[h, 2 * i + yl], i_s.at[0], i_r.at[h],
            ((z + 3 - i) % 4) * 2 + y, s,
        )

    def o_copy(h, u):
        return remote(
            inc_own.at[h], inc_all.at[h, m], o_s.at[0], o_r.at[h], mem_at(u), s
        )

    def field(h, low, w):
        with scope("field"):
            f = jnp.dot(
                coefs[h][:, :, low:low + 1024].reshape(256, 1024), basis[low:low + 1024, w],
                preferred_element_type=F32,
            )
            levels = pl.ds(h * 16, 16)
            product = f.reshape(16, 16, 1024) * anom[:, levels, w].astype(F32)
            return jnp.sum(product, axis=0)

    def near(h, i):
        w = lanes(i * 1024, 1024)
        inc_acc[h, :, w] = field(h, 1024, w)

    def far(h, i):
        w = lanes(((z + 3 - i) % 4) * 1024, 1024)
        value = (field(h, 0, w) + inc_acc[h, :, w]).astype(BF16)
        for y in range(2):
            inc_send[h, i, y] = value[:, y * 512:(y + 1) * 512]

        @pl.when(i < 3)
        def _():
            for y in range(2):
                i_copy(h, i, y).start()

        @pl.when(i == 3)
        def _():
            i_copy(h, i, 1 - yl).start()

    def reduce_own(h):
        total = inc_send[h, 3, yl].astype(F32)
        wait_all(inc_land.at[h, pl.ds(0, 7)], i_r.at[h])
        for k in range(6):
            total = total + inc_land[h, k].astype(F32)
        total = total + inc_land[h, 7 - yl].astype(F32)
        inc_own[h] = total.astype(BF16)
        for u in (5, 4, 3, 7, 1, 2, 6):
            o_copy(h, u).start()

    def near0(i, carry):
        near(0, i)

        @pl.when(i == 1)
        def _():
            with scope("rfwait"):
                came(slot_at(3))
                wait_all(landed.at[0], r_r.at[0])
            for g in range(4):
                rows = pl.ds(g * 128, 128)
                rsend[rows, :] = summed(0, rows)
            ry_copy().start()

        @pl.when(i == 3)
        def _():
            with scope("rest0wait"):
                relay_rest(0)

        return carry

    def far0(i, carry):
        far(0, i)

        @pl.when(i == 1)
        def _():
            with scope("row1wait"):
                relay_row(1)
            with scope("c1wait"):
                came(slot_at(5))
                came(slot_at(6))
                combine(1)

        return carry

    def near1(i, carry):
        near(1, i)

        @pl.when(i == 2)
        def _():
            with scope("rest1wait"):
                relay_rest(1)

        return carry

    def far1(i, carry):
        far(1, i)

        @pl.when(i == 1)
        def _():
            with scope("i0wait"):
                reduce_own(0)

        return carry

    with scope("dn0wait"):
        gathered(0, False)
    lax.fori_loop(0, 4, near0, 0)
    with scope("df0wait"):
        gathered(0, True)
    lax.fori_loop(0, 4, far0, 0)
    with scope("dn1wait"):
        gathered(1, False)
    lax.fori_loop(0, 4, near1, 0)
    with scope("rnwait"):
        came(7)
        wait_all(landed.at[1], r_r.at[1])
        ry_copy().wait_recv()
    for g in range(4):
        rows = pl.ds(g * 128, 128)
        total = summed(1, rows) + rland[rows, :]
        value = jnp.dot(rooted.T, total, precision=HIGH, preferred_element_type=F32) * gain
        spread(gall, gpair, g, value)
    depart(gall, gpair, gz_s, gz_r)
    with scope("df1wait"):
        gathered(1, True)
    lax.fori_loop(0, 4, far1, 0)

    with scope("gp1wait"):
        to_z(order, gpair, gout, gland, gz_s, gz_r)
    with scope("gz0wait"):
        to_mate(order, gall, gsend, gpart, gz_s, gz_r)
    with scope("i1wait"):
        reduce_own(1)
    for h in (1, 0):
        with scope("gs%dwait" % h):
            for i, value in arrived(order, h, gall, gsend, gpart, gland, gz_s, gz_r):
                ag_out[i, pl.ds(h * 16, 16), :] = value.astype(F32)

    for h in range(2):
        levels = pl.ds(h * 16, 16)
        inc_out[levels, lanes(m * 512, 512)] = inc_own[h].astype(F32)
        with scope("owait"):
            wait_all(inc_all.at[h, pl.ds(0, 7)], o_r.at[h])
        for u in range(1, 8):
            spot = mem_at(u)
            inc_out[levels, lanes(spot * 512, 512)] = inc_all[h, spot].astype(F32)

    with scope("sentwait"):
        for all_ref, src, dst, pair, send, recv in (
            (zall, ysend, ypart, zpair, z_s, z_r), (gall, gsend, gpart, gpair, gz_s, gz_r)
        ):
            wait_all(all_ref.at[pl.ds(0, 48)], send.at[0])
            y_copy(src, dst, send, recv).wait_send()
            pair_copy(pair, send, recv).wait_send()
            wait_all(all_ref.at[pl.ds(0, 48)], send.at[3])
        wait_all(coefs0.at[pl.ds(0, 14)], b_s.at[0])
        wait_all(coefs0, d_s.at[0])
        wait_all(inc_land.at[:, pl.ds(0, 7)], i_s.at[0])
        wait_all(inc_land.at[:, pl.ds(0, 7)], o_s.at[0])
        wait_all(relayed, rd_s.at[0])
        wait_all(landed, r_s.at[0])
        wait_all(half, x_s.at[0])
        ry_copy().wait_send()


def on_device(anomalies, alpha, basis, gradient, vertical_root, band_gain, band, order):
    vmem = pl.BlockSpec(memory_space=pltpu.VMEM)
    hbm = pl.BlockSpec(memory_space=pl.ANY)
    dma = lambda n: pltpu.SemaphoreType.DMA((n,))
    int32 = jnp.int32
    return pl.pallas_call(
        kernel,
        out_shape=(
            pltpu.VMEM((32, 4096), F32),
            pltpu.VMEM((16, 32, 128), F32),
        ),
        in_specs=[hbm] * 8,
        out_specs=(vmem, vmem),
        scratch_shapes=[
            pltpu.VMEM((1, 128), int32),
            pltpu.SMEM((1, 128), int32),
            pltpu.VMEM((8, 128), int32),
            pltpu.SMEM((8, 128), int32),
            pltpu.SMEM((1, 16), F32),
            pltpu.VMEM((16, 32, 128), BF16),
            pltpu.VMEM((32, 4096), BF16),
            pltpu.VMEM((32, 32), F32),
            pltpu.VMEM((1, 128), int32),
            pltpu.VMEM((2048, 4096), BF16),
            pltpu.VMEM((16, 32, 4096), BF16),
            pltpu.VMEM((512, 4096), BF16),
            pltpu.VMEM((8, 512, 256), F32),
            pltpu.VMEM((8, 512, 128), F32),
            pltpu.VMEM((7, 512, 128), BF16),
            pltpu.VMEM((2, 512, 128), BF16),
            pltpu.VMEM((2, 2, 512, 128), BF16),
            pltpu.VMEM((512, 128), F32),
            pltpu.VMEM((512, 128), F32),
            pltpu.VMEM((16, 16, 2048), BF16),
            pltpu.VMEM((16, 16, 2048), BF16),
            pltpu.VMEM((64, 16, 128), BF16),
            pltpu.VMEM((16, 16, 128), BF16),
            pltpu.VMEM((16, 16, 128), BF16),
            pltpu.VMEM((32, 16, 128), BF16),
            pltpu.VMEM((3, 16, 16, 128), BF16),
            pltpu.VMEM((64, 16, 128), BF16),
            pltpu.VMEM((2, 16, 4096), F32),
            pltpu.VMEM((2, 4, 2, 16, 512), BF16),
            pltpu.VMEM((2, 8, 16, 512), BF16),
            pltpu.VMEM((2, 16, 512), BF16),
            pltpu.VMEM((2, 8, 16, 512), BF16),
            pltpu.VMEM((64, 16, 128), BF16),
            pltpu.VMEM((16, 16, 128), BF16),
            pltpu.VMEM((16, 16, 128), BF16),
            pltpu.VMEM((32, 16, 128), BF16),
            pltpu.VMEM((3, 16, 16, 128), BF16),
            pltpu.VMEM((64, 16, 128), BF16),
            dma(8), dma(8), dma(4), dma(4), dma(4), dma(1), dma(2), dma(2), dma(2),
            dma(1), dma(4), dma(1), dma(8), dma(1), dma(2), dma(1), dma(2), dma(1), dma(1), dma(1),
            dma(2), dma(1), dma(2), dma(4), dma(4),
        ],
        compiler_params=pltpu.CompilerParams(
            collective_id=0, has_side_effects=True, vmem_limit_bytes=60 << 20
        ),
    )(
        order.reshape(1, -1), band_gain.reshape(1, -1), anomalies, alpha, basis, gradient,
        vertical_root, band.reshape(1, -1),
    )


def solution(mesh):
    return jax.shard_map(
        on_device,
        mesh=mesh,
        in_specs=(
            P("mem", None, "state"),
            P("mem", None, "state"),
            P(None, "state"),
            P(None, "state"),
            P(),
            P(),
            P("state"),
            P(),
        ),
        out_specs=(P(None, "state"), P("mem", None, "state")),
        check_vma=False,
    )
```

```python
import jax
import jax.numpy as jnp
from jax import lax
from jax.experimental import pallas as pl
from jax.experimental.pallas import tpu as pltpu
from jax.sharding import PartitionSpec as P

MESH = pl.DeviceIdType.MESH
NT = (((1,), (1,)), ((), ()))
HIGH = lax.Precision.HIGHEST
F32 = jnp.float32
BF16 = jnp.bfloat16
scope = jax.named_scope


def kernel(
    order_hbm, gains_hbm, anom_hbm, alpha_hbm, basis_hbm, grad_hbm, root_hbm, band_hbm,
    inc_out, ag_out,
    order_v, order, inverse_v, inverse, gains, alpha, grad, root, band,
    basis, anom, weighted, part, half, outgo, relayed, landed, rsend, rland, coefs0, coefs1,
    zall, ypart, ysend, zpair, zout, zland, inc_acc, inc_send, inc_land, inc_own, inc_all, gall, gpart, gsend, gpair, gout, gland,
    small_sem, load_sem, asem, z_s, z_r, b_s, mate_r, row_r, rest_r, d_s, d_r, x_s, x_r,
    rd_s, rd_r, r_s, r_r, ry_s, ry_r, i_s, i_r, o_s, o_r, gz_s, gz_r,
):
    coefs = (coefs0, coefs1)
    m = lax.axis_index("mem")
    s = lax.axis_index("state")
    z, yl = m // 2, m % 2
    chip, core = s // 2, s % 2
    yh, x = chip // 4, chip % 4
    other = 1 - core

    def chip_at(t):
        return ((yh + t // 4) % 2) * 4 + (x + t % 4) % 4

    def mem_at(u):
        return ((z + u // 2) % 4) * 2 + (yl + u % 2) % 2

    def remote(src, dst, send, recv, mem, state):
        return pltpu.make_async_remote_copy(
            src_ref=src, dst_ref=dst, send_sem=send, recv_sem=recv,
            device_id=(mem, state), device_id_type=MESH,
        )

    def wait_all(ref, sem):
        pltpu.make_async_copy(ref, ref, sem).wait()

    def lanes(start, width):
        return pl.ds(pl.multiple_of(start, 128), width)

    partner = chip * 2 + other
    ymate = z * 2 + (1 - yl)

    barrier = pltpu.get_barrier_semaphore()
    for u in range(1, 8):
        pl.semaphore_signal(barrier, inc=1, device_id=(mem_at(u), s), device_id_type=MESH)
    for t in range(1, 5):
        pl.semaphore_signal(
            barrier, inc=1, device_id=(m, chip_at(t) * 2 + core), device_id_type=MESH
        )
    pl.semaphore_signal(barrier, inc=1, device_id=(m, partner), device_id_type=MESH)

    def small(k):
        source, target = (
            (alpha_hbm, alpha), (root_hbm, root), (band_hbm, band), (gains_hbm, gains),
            (order_hbm, order_v), (order_hbm, order), (grad_hbm, grad),
        )[k]
        return pltpu.make_async_copy(source, target, small_sem.at[k])

    def slot_at(r):
        a, b = (r % 4) // 2, r % 2
        return (r // 4) * 4 + 3 - (2 + a - b * (1 + 2 * a))

    def load(r):
        slot = slot_at(r)
        q = chip_at(7 - slot)
        return pltpu.make_async_copy(
            basis_hbm.at[pl.ds(pl.multiple_of(q * 256, 256), 256), :],
            basis.at[pl.ds(pl.multiple_of(slot * 256, 256), 256), :],
            load_sem.at[r],
        )

    def load_anom(g):
        group = pl.ds(g * 4, 4)
        return pltpu.make_async_copy(anom_hbm.at[group], anom.at[group], asem.at[g])

    for k in range(7):
        small(k).start()
    for g in range(4):
        load_anom(g).start()
    load(0).start()
    with scope("smallwait"):
        for k in range(6):
            small(k).wait()

    bands = band[...]
    gain = jnp.zeros((1, 128), F32)
    for b in range(16):
        gain = jnp.where(bands == b, gains[0, b], gain)
    rooted = jnp.concatenate([root[...]] * 4, axis=0)
    rooted = jnp.concatenate([rooted] * 4, axis=1)
    row = lax.broadcasted_iota(jnp.int32, (128, 128), 0)
    col = lax.broadcasted_iota(jnp.int32, (128, 128), 1)
    rooted = jnp.where(row // 32 == col // 32, rooted, 0.0)

    def spread(all_ref, pair, g, value):
        value = value.astype(BF16).reshape(4, 32, 128)
        all_ref[pl.ds(z * 16 + g * 4, 4)] = value[:, :16, :]
        pair[pl.ds(yl * 16 + g * 4, 4)] = value[:, 16:, :]

    for g in range(4):
        rows = alpha[g * 4:(g + 1) * 4].astype(F32).reshape(128, 128)
        value = jnp.dot(rooted, rows, precision=HIGH, preferred_element_type=F32) * gain
        spread(zall, zpair, g, value)

    with scope("bar"):
        pl.semaphore_wait(barrier, 12)

    def z_copy(all_ref, dz, send, recv):
        mine = all_ref.at[pl.ds(z * 16, 16)]
        return remote(mine, mine, send.at[0], recv.at[0], ((z + dz) % 4) * 2 + yl, s)

    def y_copy(src, dst, send, recv):
        return remote(src, dst, send.at[1], recv.at[1], ymate, s)

    def pair_copy(pair, send, recv):
        mine = pair.at[pl.ds(yl * 16, 16)]
        return remote(mine, mine, send.at[2], recv.at[2], ymate, s)

    def out_copy(out, land, dz, send, recv):
        return remote(
            out.at[dz - 1], land.at[pl.ds(z * 16, 16)], send.at[3], recv.at[3],
            ((z + dz) % 4) * 2 + yl, s,
        )

    def depart(all_ref, pair, send, recv):
        for dz in (2, 1, 3):
            z_copy(all_ref, dz, send, recv).start()
        pair_copy(pair, send, recv).start()

    depart(zall, zpair, z_s, z_r)

    held = (order_v[...] == row).astype(F32).astype(BF16)
    slots = lax.broadcasted_iota(jnp.int32, (8, 128), 1).astype(F32).astype(BF16)
    inverse_v[...] = lax.dot_general(slots, held, NT, preferred_element_type=F32).astype(jnp.int32)
    to_scalars = pltpu.make_async_copy(inverse_v, inverse, small_sem.at[7])
    to_scalars.start()

    small(6).wait()
    for g in range(4):
        with scope("anomwait"):
            load_anom(g).wait()
        if g == 1:
            load(1).start()

        def weigh(c, carry):
            w = lanes(c * 512, 512)
            factor = grad[:, w]
            for k in range(4):
                weighted[pl.ds(g * 128 + k * 32, 32), w] = anom[g * 4 + k, :, w] * factor
            return carry

        lax.fori_loop(0, 8, weigh, 0)

    to_scalars.wait()

    def held_at(table, slot):
        return jnp.bitwise_and(table[0, slot], 127)

    def gathered_row(all_ref, where):
        return all_ref[(where // 32) * 16 + where % 16]

    def to_mate(table, all_ref, src, dst, send, recv):
        wait_all(all_ref.at[pl.ds(0, 48)], recv.at[0])
        for i in range(16):
            src[i] = gathered_row(all_ref, held_at(table, ymate * 16 + i))
        y_copy(src, dst, send, recv).start()

    def to_z(table, pair, out, land, send, recv):
        pair_copy(pair, send, recv).wait_recv()
        for dz in (2, 1, 3):
            for i in range(16):
                where = held_at(table, (((z + dz) % 4) * 2 + yl) * 16 + i)
                out[dz - 1, i] = pair[where % 32]
            out_copy(out, land, dz, send, recv).start()
        for i in range(16):
            land[z * 16 + i] = pair[held_at(table, m * 16 + i) % 32]

    def arrived(table, h, all_ref, src, dst, land, send, recv):
        if h:
            wait_all(land.at[pl.ds(0, 48)], recv.at[3])
        else:
            y_copy(src, dst, send, recv).wait_recv()
        for i in range(16):
            where = held_at(table, m * 16 + i)
            if h:
                yield i, land[(where // 32) * 16 + i]
            else:
                same = (where // 16) % 2 == yl
                yield i, jnp.where(same, gathered_row(all_ref, where), dst[i])

    def parts(h):
        return (0, 1) if h == 0 else (0,)

    def piece(h, e, r, c):
        count = 16 // len(parts(h))
        return coefs[h].at[pl.ds(e * count, count), :, lanes(r * 256 + c * 128, 128)]

    def b_copy(h, e, source, target, t, recv):
        return remote(
            piece(h, e, source, core), piece(h, e, target, core), b_s.at[0], recv.at[h],
            m, chip_at(t) * 2 + core,
        )

    def d_copy(h, e, r):
        here = piece(h, e, r, core)
        return remote(here, here, d_s.at[0], d_r.at[2 * h + r // 4], m, partner)

    def settle(h):
        for i, value in arrived(inverse, h, zall, ysend, ypart, zland, z_s, z_r):
            coefs[h][i, :, lanes(7 * 256 + core * 128, 128)] = value

    def launch_y(h):
        b_copy(h, 0, 7, 3, 4, mate_r).start()
        if h == 0:
            b_copy(h, 1, 7, 3, 4, rest_r).start()
        for e in parts(h):
            d_copy(h, e, 7).start()

    def launch_x(h):
        for dx in (2, 1, 3):
            for e in parts(h):
                b_copy(h, e, 7, 3 + dx, dx, row_r).start()

    def relay_mate(h):
        wait_all(piece(h, 0, 3, core), mate_r.at[h])
        for dx in (2, 1, 3):
            b_copy(h, 0, 3, dx - 1, dx, rest_r).start()
        d_copy(h, 0, 3).start()

    def relay_row(h):
        wait_all(coefs[h].at[pl.ds(0, 3)], row_r.at[h])
        for dx in (1, 3, 2):
            if h == 0:
                b_copy(h, 1, 7 - dx, 3 - dx, 4, rest_r).start()
            for e in parts(h):
                d_copy(h, e, 7 - dx).start()

    def relay_rest(h):
        if h == 0:
            wait_all(coefs[h].at[pl.ds(0, 7), :, pl.ds(0, 1024)], rest_r.at[h])
            d_copy(h, 1, 3).start()
        else:
            wait_all(coefs[h].at[pl.ds(0, 3)], rest_r.at[h])
        for r in range(3):
            for e in parts(h):
                d_copy(h, e, r).start()

    def gathered(h, far):
        wait_all(coefs[h].at[pl.ds(0, 4)], d_r.at[2 * h + 1 - far])

    def x_copy(r):
        return remote(
            part.at[r, :, lanes(other * 128, 128)], half.at[r], x_s.at[0], x_r.at[r], m, partner
        )

    def came(slot):
        x_copy(slot).wait_recv()

    def rd_copy(g, side):
        rows = pl.ds(side * 256, 256)
        return remote(
            outgo.at[4 * g + 1, rows], relayed.at[g, rows], rd_s.at[0], rd_r.at[g], m,
            chip_at(1 + 2 * side) * 2 + core,
        )

    def r_copy(g, side, rows):
        slot = 4 * g + 2 - 2 * side
        return remote(
            outgo.at[slot, rows], landed.at[g, side, rows], r_s.at[0], r_r.at[g], m,
            chip_at(1 + 2 * side) * 2 + core,
        )

    def pass_half(g):
        slot = 4 * g + 1
        outgo[slot] = own(slot, pl.ds(0, 512)).astype(BF16)
        for side in range(2):
            rd_copy(g, side).start()

    def alone(g, side):
        slot = 4 * g + 2 - 2 * side
        rows = pl.ds((1 - side) * 256, 256)
        outgo[slot, rows, :] = own(slot, rows).astype(BF16)
        r_copy(g, side, rows).start()

    def combine(g):
        wait_all(relayed.at[g], rd_r.at[g])
        for side in range(2):
            slot = 4 * g + 2 - 2 * side
            rows = pl.ds(side * 256, 256)
            total = own(slot, rows) + relayed[g, rows, :].astype(F32)
            outgo[slot, rows, :] = total.astype(BF16)
            r_copy(g, side, rows).start()

    def summed(g, rows):
        total = own(4 * g + 3, rows)
        for side in range(2):
            total = total + landed[g, side, rows, :].astype(F32)
        return total

    def ry_copy():
        return remote(rsend, rland, ry_s.at[0], ry_r.at[0], m, chip_at(4) * 2 + core)

    def own(r, rows):
        return part[r, rows, lanes(core * 128, 128)] + half[r, rows, :]

    def adjoint(r, carry):
        @pl.when(r < 6)
        def _():
            load(r + 2).start()

        with scope("bwait"):
            load(r).wait()
        slot = slot_at(r)
        rows = pl.ds(pl.multiple_of(slot * 256, 256), 256)
        with scope("adot"):
            part[slot] = lax.dot_general(
                weighted[...], basis[rows, :], NT, preferred_element_type=F32
            )
        x_copy(slot).start()

        @pl.when(r == 1)
        def _():
            with scope("z0wait"):
                to_mate(inverse, zall, ysend, ypart, z_s, z_r)
            with scope("xwait"):
                came(slot_at(0))
            pass_half(0)
            with scope("p1wait"):
                to_z(inverse, zpair, zout, zland, z_s, z_r)

        @pl.when(r == 2)
        def _():
            came(slot_at(1))
            alone(0, 0)

        @pl.when(r == 3)
        def _():
            came(slot_at(2))
            alone(0, 1)
            with scope("s0wait"):
                settle(0)
            launch_y(0)
            launch_x(0)
            with scope("c0wait"):
                combine(0)

        @pl.when(r == 4)
        def _():
            with scope("s1wait"):
                settle(1)
            launch_y(1)

        @pl.when(r == 5)
        def _():
            with scope("mate0wait"):
                relay_mate(0)
            launch_x(1)
            with scope("xwait"):
                came(slot_at(4))
            pass_half(1)

        @pl.when(r == 6)
        def _():
            with scope("row0wait"):
                relay_row(0)

        return carry

    lax.fori_loop(0, 8, adjoint, 0)
    with scope("mate1wait"):
        relay_mate(1)
    for side in range(2):
        came(slot_at(5 + side))
        alone(1, side)

    def i_copy(h, i, y):
        return remote(
            inc_send.at[h, i, y], inc_land.at[h, 2 * i + yl], i_s.at[0], i_r.at[h],
            ((z + 3 - i) % 4) * 2 + y, s,
        )

    def o_copy(h, u):
        return remote(
            inc_own.at[h], inc_all.at[h, m], o_s.at[0], o_r.at[h], mem_at(u), s
        )

    def field(h, low, w):
        with scope("field"):
            f = jnp.dot(
                coefs[h][:, :, low:low + 1024].reshape(256, 1024), basis[low:low + 1024, w],
                preferred_element_type=F32,
            )
            levels = pl.ds(h * 16, 16)
            product = f.reshape(16, 16, 1024) * anom[:, levels, w].astype(F32)
            return jnp.sum(product, axis=0)

    def near(h, i):
        w = lanes(i * 1024, 1024)
        inc_acc[h, :, w] = field(h, 1024, w)

    def far(h, i):
        w = lanes(((z + 3 - i) % 4) * 1024, 1024)
        value = (field(h, 0, w) + inc_acc[h, :, w]).astype(BF16)
        for y in range(2):
            inc_send[h, i, y] = value[:, y * 512:(y + 1) * 512]

        @pl.when(i < 3)
        def _():
            for y in range(2):
                i_copy(h, i, y).start()

        @pl.when(i == 3)
        def _():
            i_copy(h, i, 1 - yl).start()

    def reduce_own(h):
        total = inc_send[h, 3, yl].astype(F32)
        wait_all(inc_land.at[h, pl.ds(0, 7)], i_r.at[h])
        for k in range(6):
            total = total + inc_land[h, k].astype(F32)
        total = total + inc_land[h, 7 - yl].astype(F32)
        inc_own[h] = total.astype(BF16)
        for u in (5, 4, 3, 7, 1, 2, 6):
            o_copy(h, u).start()

    def near0(i, carry):
        near(0, i)

        @pl.when(i == 1)
        def _():
            with scope("rfwait"):
                came(slot_at(3))
                wait_all(landed.at[0], r_r.at[0])
            for g in range(4):
                rows = pl.ds(g * 128, 128)
                rsend[rows, :] = summed(0, rows)
            ry_copy().start()

        @pl.when(i == 3)
        def _():
            with scope("rest0wait"):
                relay_rest(0)

        return carry

    def far0(i, carry):
        far(0, i)

        @pl.when(i == 1)
        def _():
            with scope("row1wait"):
                relay_row(1)
            with scope("c1wait"):
                combine(1)

        return carry

    def near1(i, carry):
        near(1, i)

        @pl.when(i == 2)
        def _():
            with scope("rest1wait"):
                relay_rest(1)

        @pl.when(i == 2)
        def _():
            with scope("rnwait"):
                came(7)
                wait_all(landed.at[1], r_r.at[1])
                ry_copy().wait_recv()
            for g in range(4):
                rows = pl.ds(g * 128, 128)
                total = summed(1, rows) + rland[rows, :]
                value = jnp.dot(rooted.T, total, precision=HIGH, preferred_element_type=F32) * gain
                spread(gall, gpair, g, value)
            depart(gall, gpair, gz_s, gz_r)

        return carry

    def far1(i, carry):
        far(1, i)

        @pl.when(i == 1)
        def _():
            with scope("i0wait"):
                reduce_own(0)

        return carry

    with scope("dn0wait"):
        gathered(0, False)
    lax.fori_loop(0, 4, near0, 0)
    with scope("df0wait"):
        gathered(0, True)
    lax.fori_loop(0, 4, far0, 0)
    with scope("dn1wait"):
        gathered(1, False)
    lax.fori_loop(0, 4, near1, 0)
    with scope("df1wait"):
        gathered(1, True)
    lax.fori_loop(0, 4, far1, 0)

    with scope("gp1wait"):
        to_z(order, gpair, gout, gland, gz_s, gz_r)
    with scope("gz0wait"):
        to_mate(order, gall, gsend, gpart, gz_s, gz_r)
    with scope("i1wait"):
        reduce_own(1)
    for h in (1, 0):
        with scope("gs%dwait" % h):
            for i, value in arrived(order, h, gall, gsend, gpart, gland, gz_s, gz_r):
                ag_out[i, pl.ds(h * 16, 16), :] = value.astype(F32)

    for h in range(2):
        levels = pl.ds(h * 16, 16)
        inc_out[levels, lanes(m * 512, 512)] = inc_own[h].astype(F32)
        with scope("owait"):
            wait_all(inc_all.at[h, pl.ds(0, 7)], o_r.at[h])
        for u in range(1, 8):
            spot = mem_at(u)
            inc_out[levels, lanes(spot * 512, 512)] = inc_all[h, spot].astype(F32)

    with scope("sentwait"):
        for all_ref, src, dst, pair, send, recv in (
            (zall, ysend, ypart, zpair, z_s, z_r), (gall, gsend, gpart, gpair, gz_s, gz_r)
        ):
            wait_all(all_ref.at[pl.ds(0, 48)], send.at[0])
            y_copy(src, dst, send, recv).wait_send()
            pair_copy(pair, send, recv).wait_send()
            wait_all(all_ref.at[pl.ds(0, 48)], send.at[3])
        wait_all(coefs0.at[pl.ds(0, 14)], b_s.at[0])
        wait_all(coefs0, d_s.at[0])
        wait_all(inc_land.at[:, pl.ds(0, 7)], i_s.at[0])
        wait_all(inc_land.at[:, pl.ds(0, 7)], o_s.at[0])
        wait_all(relayed, rd_s.at[0])
        wait_all(landed, r_s.at[0])
        wait_all(half, x_s.at[0])
        ry_copy().wait_send()


def write_out(inc, ag, inc_out, ag_out, sem):
    copies = [
        pltpu.make_async_copy(inc, inc_out, sem.at[0]),
        pltpu.make_async_copy(ag, ag_out, sem.at[1]),
    ]
    for copy in copies:
        copy.start()
    for copy in copies:
        copy.wait()


def on_device(anomalies, alpha, basis, gradient, vertical_root, band_gain, band, order):
    vmem = pl.BlockSpec(memory_space=pltpu.VMEM)
    hbm = pl.BlockSpec(memory_space=pl.ANY)
    dma = lambda n: pltpu.SemaphoreType.DMA((n,))
    int32 = jnp.int32
    inc, ag = pl.pallas_call(
        kernel,
        out_shape=(
            pltpu.VMEM((32, 4096), F32),
            pltpu.VMEM((16, 32, 128), F32),
        ),
        in_specs=[hbm] * 8,
        out_specs=(vmem, vmem),
        scratch_shapes=[
            pltpu.VMEM((1, 128), int32),
            pltpu.SMEM((1, 128), int32),
            pltpu.VMEM((8, 128), int32),
            pltpu.SMEM((8, 128), int32),
            pltpu.SMEM((1, 16), F32),
            pltpu.VMEM((16, 32, 128), BF16),
            pltpu.VMEM((32, 4096), BF16),
            pltpu.VMEM((32, 32), F32),
            pltpu.VMEM((1, 128), int32),
            pltpu.VMEM((2048, 4096), BF16),
            pltpu.VMEM((16, 32, 4096), BF16),
            pltpu.VMEM((512, 4096), BF16),
            pltpu.VMEM((8, 512, 256), F32),
            pltpu.VMEM((8, 512, 128), F32),
            pltpu.VMEM((7, 512, 128), BF16),
            pltpu.VMEM((2, 512, 128), BF16),
            pltpu.VMEM((2, 2, 512, 128), BF16),
            pltpu.VMEM((512, 128), F32),
            pltpu.VMEM((512, 128), F32),
            pltpu.VMEM((16, 16, 2048), BF16),
            pltpu.VMEM((16, 16, 2048), BF16),
            pltpu.VMEM((64, 16, 128), BF16),
            pltpu.VMEM((16, 16, 128), BF16),
            pltpu.VMEM((16, 16, 128), BF16),
            pltpu.VMEM((32, 16, 128), BF16),
            pltpu.VMEM((3, 16, 16, 128), BF16),
            pltpu.VMEM((64, 16, 128), BF16),
            pltpu.VMEM((2, 16, 4096), F32),
            pltpu.VMEM((2, 4, 2, 16, 512), BF16),
            pltpu.VMEM((2, 8, 16, 512), BF16),
            pltpu.VMEM((2, 16, 512), BF16),
            pltpu.VMEM((2, 8, 16, 512), BF16),
            pltpu.VMEM((64, 16, 128), BF16),
            pltpu.VMEM((16, 16, 128), BF16),
            pltpu.VMEM((16, 16, 128), BF16),
            pltpu.VMEM((32, 16, 128), BF16),
            pltpu.VMEM((3, 16, 16, 128), BF16),
            pltpu.VMEM((64, 16, 128), BF16),
            dma(8), dma(8), dma(4), dma(4), dma(4), dma(1), dma(2), dma(2), dma(2),
            dma(1), dma(4), dma(1), dma(8), dma(1), dma(2), dma(1), dma(2), dma(1), dma(1), dma(1),
            dma(2), dma(1), dma(2), dma(4), dma(4),
        ],
        compiler_params=pltpu.CompilerParams(
            collective_id=0, has_side_effects=True, vmem_limit_bytes=60 << 20
        ),
    )(
        order.reshape(1, -1), band_gain.reshape(1, -1), anomalies, alpha, basis, gradient,
        vertical_root, band.reshape(1, -1),
    )
    inc = pltpu.with_memory_space_constraint(inc, pltpu.VMEM)
    ag = pltpu.with_memory_space_constraint(ag, pltpu.VMEM)
    return pl.pallas_call(
        write_out,
        out_shape=(
            jax.ShapeDtypeStruct((32, 4096), F32),
            jax.ShapeDtypeStruct((16, 32, 128), F32),
        ),
        in_specs=[vmem] * 2,
        out_specs=(hbm, hbm),
        scratch_shapes=[dma(2)],
    )(inc, ag)


def solution(mesh):
    return jax.shard_map(
        on_device,
        mesh=mesh,
        in_specs=(
            P("mem", None, "state"),
            P("mem", None, "state"),
            P(None, "state"),
            P(None, "state"),
            P(),
            P(),
            P("state"),
            P(),
        ),
        out_specs=(P(None, "state"), P("mem", None, "state")),
        check_vma=False,
    )
```

```python
import jax
import jax.numpy as jnp
from jax import lax
from jax.experimental import pallas as pl
from jax.experimental.pallas import tpu as pltpu
from jax.sharding import PartitionSpec as P

MESH = pl.DeviceIdType.MESH
NT = (((1,), (1,)), ((), ()))
HIGH = lax.Precision.HIGHEST
F32 = jnp.float32
BF16 = jnp.bfloat16
scope = jax.named_scope


def kernel(
    order_hbm, gains_hbm, anom_hbm, alpha_hbm, basis_hbm, grad_hbm, root_hbm, band_hbm,
    inc_out, ag_out,
    order_v, order, inverse_v, inverse, gains, alpha, grad, root, band,
    basis, anom, weighted, part, half, outgo, relayed, landed, rsend, rland, coefs0, coefs1,
    zall, ypart, ysend, zpair, zout, zland, inc_acc, inc_send, inc_land, inc_own, inc_all, gall, gpart, gsend, gpair, gout, gland,
    small_sem, load_sem, asem, z_s, z_r, b_s, mate_r, row_r, rest_r, d_s, d_r, x_s, x_r,
    rd_s, rd_r, r_s, r_r, ry_s, ry_r, i_s, i_r, o_s, o_r, gz_s, gz_r,
):
    coefs = (coefs0, coefs1)
    m = lax.axis_index("mem")
    s = lax.axis_index("state")
    z, yl = m // 2, m % 2
    chip, core = s // 2, s % 2
    yh, x = chip // 4, chip % 4
    other = 1 - core

    def chip_at(t):
        return ((yh + t // 4) % 2) * 4 + (x + t % 4) % 4

    def mem_at(u):
        return ((z + u // 2) % 4) * 2 + (yl + u % 2) % 2

    def remote(src, dst, send, recv, mem, state):
        return pltpu.make_async_remote_copy(
            src_ref=src, dst_ref=dst, send_sem=send, recv_sem=recv,
            device_id=(mem, state), device_id_type=MESH,
        )

    def wait_all(ref, sem):
        pltpu.make_async_copy(ref, ref, sem).wait()

    def lanes(start, width):
        return pl.ds(pl.multiple_of(start, 128), width)

    partner = chip * 2 + other
    ymate = z * 2 + (1 - yl)

    barrier = pltpu.get_barrier_semaphore()
    for u in range(1, 8):
        pl.semaphore_signal(barrier, inc=1, device_id=(mem_at(u), s), device_id_type=MESH)
    for t in range(1, 5):
        pl.semaphore_signal(
            barrier, inc=1, device_id=(m, chip_at(t) * 2 + core), device_id_type=MESH
        )
    pl.semaphore_signal(barrier, inc=1, device_id=(m, partner), device_id_type=MESH)

    def small(k):
        source, target = (
            (alpha_hbm, alpha), (root_hbm, root), (band_hbm, band), (gains_hbm, gains),
            (order_hbm, order_v), (order_hbm, order), (grad_hbm, grad),
        )[k]
        return pltpu.make_async_copy(source, target, small_sem.at[k])

    def slot_at(r):
        a, b = (r % 4) // 2, r % 2
        return (r // 4) * 4 + 3 - (2 + a - b * (1 + 2 * a))

    def load(r):
        slot = slot_at(r)
        q = chip_at(7 - slot)
        return pltpu.make_async_copy(
            basis_hbm.at[pl.ds(pl.multiple_of(q * 256, 256), 256), :],
            basis.at[pl.ds(pl.multiple_of(slot * 256, 256), 256), :],
            load_sem.at[r],
        )

    def load_anom(g):
        group = pl.ds(g * 4, 4)
        return pltpu.make_async_copy(anom_hbm.at[group], anom.at[group], asem.at[g])

    for k in range(7):
        small(k).start()
    for g in range(4):
        load_anom(g).start()
    load(0).start()
    with scope("smallwait"):
        for k in range(6):
            small(k).wait()

    bands = band[...]
    gain = jnp.zeros((1, 128), F32)
    for b in range(16):
        gain = jnp.where(bands == b, gains[0, b], gain)
    rooted = jnp.concatenate([root[...]] * 4, axis=0)
    rooted = jnp.concatenate([rooted] * 4, axis=1)
    row = lax.broadcasted_iota(jnp.int32, (128, 128), 0)
    col = lax.broadcasted_iota(jnp.int32, (128, 128), 1)
    rooted = jnp.where(row // 32 == col // 32, rooted, 0.0)

    def spread(all_ref, pair, g, value):
        value = value.astype(BF16).reshape(4, 32, 128)
        all_ref[pl.ds(z * 16 + g * 4, 4)] = value[:, :16, :]
        pair[pl.ds(yl * 16 + g * 4, 4)] = value[:, 16:, :]

    for g in range(4):
        rows = alpha[g * 4:(g + 1) * 4].astype(F32).reshape(128, 128)
        value = jnp.dot(rooted, rows, precision=HIGH, preferred_element_type=F32) * gain
        spread(zall, zpair, g, value)

    with scope("bar"):
        pl.semaphore_wait(barrier, 12)

    def z_copy(all_ref, dz, send, recv):
        mine = all_ref.at[pl.ds(z * 16, 16)]
        return remote(mine, mine, send.at[0], recv.at[0], ((z + dz) % 4) * 2 + yl, s)

    def y_copy(src, dst, send, recv):
        return remote(src, dst, send.at[1], recv.at[1], ymate, s)

    def pair_copy(pair, send, recv):
        mine = pair.at[pl.ds(yl * 16, 16)]
        return remote(mine, mine, send.at[2], recv.at[2], ymate, s)

    def out_copy(out, land, dz, send, recv):
        return remote(
            out.at[dz - 1], land.at[pl.ds(z * 16, 16)], send.at[3], recv.at[3],
            ((z + dz) % 4) * 2 + yl, s,
        )

    def depart(all_ref, pair, send, recv):
        for dz in (2, 1, 3):
            z_copy(all_ref, dz, send, recv).start()
        pair_copy(pair, send, recv).start()

    depart(zall, zpair, z_s, z_r)

    held = (order_v[...] == row).astype(F32).astype(BF16)
    slots = lax.broadcasted_iota(jnp.int32, (8, 128), 1).astype(F32).astype(BF16)
    inverse_v[...] = lax.dot_general(slots, held, NT, preferred_element_type=F32).astype(jnp.int32)
    to_scalars = pltpu.make_async_copy(inverse_v, inverse, small_sem.at[7])
    to_scalars.start()

    small(6).wait()
    for g in range(4):
        with scope("anomwait"):
            load_anom(g).wait()
        if g == 1:
            load(1).start()

        def weigh(c, carry):
            w = lanes(c * 512, 512)
            factor = grad[:, w]
            for k in range(4):
                weighted[pl.ds(g * 128 + k * 32, 32), w] = anom[g * 4 + k, :, w] * factor
            return carry

        lax.fori_loop(0, 8, weigh, 0)

    to_scalars.wait()

    def held_at(table, slot):
        return jnp.bitwise_and(table[0, slot], 127)

    def gathered_row(all_ref, where):
        return all_ref[(where // 32) * 16 + where % 16]

    def to_mate(table, all_ref, src, dst, send, recv):
        wait_all(all_ref.at[pl.ds(0, 48)], recv.at[0])
        for i in range(16):
            src[i] = gathered_row(all_ref, held_at(table, ymate * 16 + i))
        y_copy(src, dst, send, recv).start()

    def to_z(table, pair, out, land, send, recv):
        pair_copy(pair, send, recv).wait_recv()
        for dz in (2, 1, 3):
            for i in range(16):
                where = held_at(table, (((z + dz) % 4) * 2 + yl) * 16 + i)
                out[dz - 1, i] = pair[where % 32]
            out_copy(out, land, dz, send, recv).start()
        for i in range(16):
            land[z * 16 + i] = pair[held_at(table, m * 16 + i) % 32]

    def arrived(table, h, all_ref, src, dst, land, send, recv):
        if h:
            wait_all(land.at[pl.ds(0, 48)], recv.at[3])
        else:
            y_copy(src, dst, send, recv).wait_recv()
        for i in range(16):
            where = held_at(table, m * 16 + i)
            if h:
                yield i, land[(where // 32) * 16 + i]
            else:
                same = (where // 16) % 2 == yl
                yield i, jnp.where(same, gathered_row(all_ref, where), dst[i])

    def parts(h):
        return (0, 1) if h == 0 else (0,)

    def piece(h, e, r, c):
        count = 16 // len(parts(h))
        return coefs[h].at[pl.ds(e * count, count), :, lanes(r * 256 + c * 128, 128)]

    def b_copy(h, e, source, target, t, recv):
        return remote(
            piece(h, e, source, core), piece(h, e, target, core), b_s.at[0], recv.at[h],
            m, chip_at(t) * 2 + core,
        )

    def d_copy(h, e, r):
        here = piece(h, e, r, core)
        return remote(here, here, d_s.at[0], d_r.at[2 * h + r // 4], m, partner)

    def settle(h):
        for i, value in arrived(inverse, h, zall, ysend, ypart, zland, z_s, z_r):
            coefs[h][i, :, lanes(7 * 256 + core * 128, 128)] = value

    def launch_y(h):
        b_copy(h, 0, 7, 3, 4, mate_r).start()
        if h == 0:
            b_copy(h, 1, 7, 3, 4, rest_r).start()
        for e in parts(h):
            d_copy(h, e, 7).start()

    def launch_x(h):
        for dx in (2, 1, 3):
            for e in parts(h):
                b_copy(h, e, 7, 3 + dx, dx, row_r).start()

    def relay_mate(h):
        wait_all(piece(h, 0, 3, core), mate_r.at[h])
        for dx in (2, 1, 3):
            b_copy(h, 0, 3, dx - 1, dx, rest_r).start()
        d_copy(h, 0, 3).start()

    def relay_row(h):
        wait_all(coefs[h].at[pl.ds(0, 3)], row_r.at[h])
        for dx in (1, 3, 2):
            if h == 0:
                b_copy(h, 1, 7 - dx, 3 - dx, 4, rest_r).start()
            for e in parts(h):
                d_copy(h, e, 7 - dx).start()

    def relay_rest(h):
        if h == 0:
            wait_all(coefs[h].at[pl.ds(0, 7), :, pl.ds(0, 1024)], rest_r.at[h])
            d_copy(h, 1, 3).start()
        else:
            wait_all(coefs[h].at[pl.ds(0, 3)], rest_r.at[h])
        for r in range(3):
            for e in parts(h):
                d_copy(h, e, r).start()

    def gathered(h, far):
        wait_all(coefs[h].at[pl.ds(0, 4)], d_r.at[2 * h + 1 - far])

    def x_copy(r):
        return remote(
            part.at[r, :, lanes(other * 128, 128)], half.at[r], x_s.at[0], x_r.at[r], m, partner
        )

    def came(slot):
        x_copy(slot).wait_recv()

    def rd_copy(g, side):
        rows = pl.ds(side * 256, 256)
        return remote(
            outgo.at[4 * g + 1, rows], relayed.at[g, rows], rd_s.at[0], rd_r.at[g], m,
            chip_at(1 + 2 * side) * 2 + core,
        )

    def r_copy(g, side, rows):
        slot = 4 * g + 2 - 2 * side
        return remote(
            outgo.at[slot, rows], landed.at[g, side, rows], r_s.at[0], r_r.at[g], m,
            chip_at(1 + 2 * side) * 2 + core,
        )

    def pass_half(g):
        slot = 4 * g + 1
        outgo[slot] = own(slot, pl.ds(0, 512)).astype(BF16)
        for side in range(2):
            rd_copy(g, side).start()

    def alone(g, side):
        slot = 4 * g + 2 - 2 * side
        rows = pl.ds((1 - side) * 256, 256)
        outgo[slot, rows, :] = own(slot, rows).astype(BF16)
        r_copy(g, side, rows).start()

    def combine(g):
        wait_all(relayed.at[g], rd_r.at[g])
        for side in range(2):
            slot = 4 * g + 2 - 2 * side
            rows = pl.ds(side * 256, 256)
            total = own(slot, rows) + relayed[g, rows, :].astype(F32)
            outgo[slot, rows, :] = total.astype(BF16)
            r_copy(g, side, rows).start()

    def summed(g, rows):
        total = own(4 * g + 3, rows)
        for side in range(2):
            total = total + landed[g, side, rows, :].astype(F32)
        return total

    def ry_copy():
        return remote(rsend, rland, ry_s.at[0], ry_r.at[0], m, chip_at(4) * 2 + core)

    def own(r, rows):
        return part[r, rows, lanes(core * 128, 128)] + half[r, rows, :]

    def adjoint(r, carry):
        @pl.when(r < 6)
        def _():
            load(r + 2).start()

        with scope("bwait"):
            load(r).wait()
        slot = slot_at(r)
        rows = pl.ds(pl.multiple_of(slot * 256, 256), 256)
        with scope("adot"):
            part[slot] = lax.dot_general(
                weighted[...], basis[rows, :], NT, preferred_element_type=F32
            )
        x_copy(slot).start()

        @pl.when(r == 1)
        def _():
            with scope("z0wait"):
                to_mate(inverse, zall, ysend, ypart, z_s, z_r)
            with scope("xwait"):
                came(slot_at(0))
            pass_half(0)
            with scope("p1wait"):
                to_z(inverse, zpair, zout, zland, z_s, z_r)

        @pl.when(r == 2)
        def _():
            came(slot_at(1))
            alone(0, 0)

        @pl.when(r == 3)
        def _():
            came(slot_at(2))
            alone(0, 1)
            with scope("s0wait"):
                settle(0)
            launch_y(0)
            launch_x(0)
            with scope("c0wait"):
                combine(0)

        @pl.when(r == 4)
        def _():
            with scope("s1wait"):
                settle(1)
            launch_y(1)

        @pl.when(r == 5)
        def _():
            with scope("mate0wait"):
                relay_mate(0)
            launch_x(1)
            with scope("xwait"):
                came(slot_at(4))
            pass_half(1)

        @pl.when(r == 6)
        def _():
            with scope("row0wait"):
                relay_row(0)

        return carry

    lax.fori_loop(0, 8, adjoint, 0)
    with scope("mate1wait"):
        relay_mate(1)
    for side in range(2):
        came(slot_at(5 + side))
        alone(1, side)

    def i_copy(h, i, y):
        return remote(
            inc_send.at[h, i, y], inc_land.at[h, 2 * i + yl], i_s.at[0], i_r.at[h],
            ((z + 3 - i) % 4) * 2 + y, s,
        )

    def o_copy(h, u):
        return remote(
            inc_own.at[h], inc_all.at[h, m], o_s.at[0], o_r.at[h], mem_at(u), s
        )

    def field(h, low, w):
        with scope("field"):
            f = jnp.dot(
                coefs[h][:, :, low:low + 1024].reshape(256, 1024), basis[low:low + 1024, w],
                preferred_element_type=F32,
            )
            levels = pl.ds(h * 16, 16)
            product = f.reshape(16, 16, 1024) * anom[:, levels, w].astype(F32)
            return jnp.sum(product, axis=0)

    def near(h, i):
        w = lanes(i * 1024, 1024)
        inc_acc[h, :, w] = field(h, 1024, w)

    def far(h, i):
        w = lanes(((z + 3 - i) % 4) * 1024, 1024)
        value = (field(h, 0, w) + inc_acc[h, :, w]).astype(BF16)
        for y in range(2):
            inc_send[h, i, y] = value[:, y * 512:(y + 1) * 512]

        @pl.when(i < 3)
        def _():
            for y in range(2):
                i_copy(h, i, y).start()

        @pl.when(i == 3)
        def _():
            i_copy(h, i, 1 - yl).start()

    def reduce_own(h):
        total = inc_send[h, 3, yl].astype(F32)
        wait_all(inc_land.at[h, pl.ds(0, 7)], i_r.at[h])
        for k in range(6):
            total = total + inc_land[h, k].astype(F32)
        total = total + inc_land[h, 7 - yl].astype(F32)
        inc_own[h] = total.astype(BF16)
        for u in (5, 4, 3, 7, 1, 2, 6):
            o_copy(h, u).start()

    def near0(i, carry):
        near(0, i)

        @pl.when(i == 1)
        def _():
            with scope("rfwait"):
                came(slot_at(3))
                wait_all(landed.at[0], r_r.at[0])
            for g in range(4):
                rows = pl.ds(g * 128, 128)
                rsend[rows, :] = summed(0, rows)
            ry_copy().start()

        @pl.when(i == 2)
        def _():
            with scope("rest0wait"):
                relay_rest(0)

        return carry

    def far0(i, carry):
        far(0, i)

        @pl.when(i == 1)
        def _():
            with scope("row1wait"):
                relay_row(1)
            with scope("c1wait"):
                combine(1)

        return carry

    def near1(i, carry):
        near(1, i)

        @pl.when(i == 2)
        def _():
            with scope("rest1wait"):
                relay_rest(1)

        @pl.when(i == 2)
        def _():
            with scope("rnwait"):
                came(7)
                wait_all(landed.at[1], r_r.at[1])
                ry_copy().wait_recv()
            for g in range(4):
                rows = pl.ds(g * 128, 128)
                total = summed(1, rows) + rland[rows, :]
                value = jnp.dot(rooted.T, total, precision=HIGH, preferred_element_type=F32) * gain
                spread(gall, gpair, g, value)
            depart(gall, gpair, gz_s, gz_r)

        return carry

    def far1(i, carry):
        far(1, i)

        @pl.when(i == 1)
        def _():
            with scope("i0wait"):
                reduce_own(0)

        return carry

    with scope("dn0wait"):
        gathered(0, False)
    lax.fori_loop(0, 4, near0, 0)
    with scope("df0wait"):
        gathered(0, True)
    lax.fori_loop(0, 4, far0, 0)
    with scope("dn1wait"):
        gathered(1, False)
    lax.fori_loop(0, 4, near1, 0)
    with scope("df1wait"):
        gathered(1, True)
    lax.fori_loop(0, 4, far1, 0)

    with scope("gp1wait"):
        to_z(order, gpair, gout, gland, gz_s, gz_r)
    with scope("gz0wait"):
        to_mate(order, gall, gsend, gpart, gz_s, gz_r)
    with scope("i1wait"):
        reduce_own(1)
    for h in (1, 0):
        with scope("gs%dwait" % h):
            for i, value in arrived(order, h, gall, gsend, gpart, gland, gz_s, gz_r):
                ag_out[i, pl.ds(h * 16, 16), :] = value.astype(F32)

    for h in range(2):
        levels = pl.ds(h * 16, 16)
        inc_out[levels, lanes(m * 512, 512)] = inc_own[h].astype(F32)
        with scope("owait"):
            wait_all(inc_all.at[h, pl.ds(0, 7)], o_r.at[h])
        for u in range(1, 8):
            spot = mem_at(u)
            inc_out[levels, lanes(spot * 512, 512)] = inc_all[h, spot].astype(F32)

    with scope("sentwait"):
        for all_ref, src, dst, pair, send, recv in (
            (zall, ysend, ypart, zpair, z_s, z_r), (gall, gsend, gpart, gpair, gz_s, gz_r)
        ):
            wait_all(all_ref.at[pl.ds(0, 48)], send.at[0])
            y_copy(src, dst, send, recv).wait_send()
            pair_copy(pair, send, recv).wait_send()
            wait_all(all_ref.at[pl.ds(0, 48)], send.at[3])
        wait_all(coefs0.at[pl.ds(0, 14)], b_s.at[0])
        wait_all(coefs0, d_s.at[0])
        wait_all(inc_land.at[:, pl.ds(0, 7)], i_s.at[0])
        wait_all(inc_land.at[:, pl.ds(0, 7)], o_s.at[0])
        wait_all(relayed, rd_s.at[0])
        wait_all(landed, r_s.at[0])
        wait_all(half, x_s.at[0])
        ry_copy().wait_send()


def write_out(inc, ag, inc_out, ag_out, sem):
    copies = [
        pltpu.make_async_copy(inc, inc_out, sem.at[0]),
        pltpu.make_async_copy(ag, ag_out, sem.at[1]),
    ]
    for copy in copies:
        copy.start()
    for copy in copies:
        copy.wait()


def on_device(anomalies, alpha, basis, gradient, vertical_root, band_gain, band, order):
    vmem = pl.BlockSpec(memory_space=pltpu.VMEM)
    hbm = pl.BlockSpec(memory_space=pl.ANY)
    dma = lambda n: pltpu.SemaphoreType.DMA((n,))
    int32 = jnp.int32
    inc, ag = pl.pallas_call(
        kernel,
        out_shape=(
            pltpu.VMEM((32, 4096), F32),
            pltpu.VMEM((16, 32, 128), F32),
        ),
        in_specs=[hbm] * 8,
        out_specs=(vmem, vmem),
        scratch_shapes=[
            pltpu.VMEM((1, 128), int32),
            pltpu.SMEM((1, 128), int32),
            pltpu.VMEM((8, 128), int32),
            pltpu.SMEM((8, 128), int32),
            pltpu.SMEM((1, 16), F32),
            pltpu.VMEM((16, 32, 128), BF16),
            pltpu.VMEM((32, 4096), BF16),
            pltpu.VMEM((32, 32), F32),
            pltpu.VMEM((1, 128), int32),
            pltpu.VMEM((2048, 4096), BF16),
            pltpu.VMEM((16, 32, 4096), BF16),
            pltpu.VMEM((512, 4096), BF16),
            pltpu.VMEM((8, 512, 256), F32),
            pltpu.VMEM((8, 512, 128), F32),
            pltpu.VMEM((7, 512, 128), BF16),
            pltpu.VMEM((2, 512, 128), BF16),
            pltpu.VMEM((2, 2, 512, 128), BF16),
            pltpu.VMEM((512, 128), F32),
            pltpu.VMEM((512, 128), F32),
            pltpu.VMEM((16, 16, 2048), BF16),
            pltpu.VMEM((16, 16, 2048), BF16),
            pltpu.VMEM((64, 16, 128), BF16),
            pltpu.VMEM((16, 16, 128), BF16),
            pltpu.VMEM((16, 16, 128), BF16),
            pltpu.VMEM((32, 16, 128), BF16),
            pltpu.VMEM((3, 16, 16, 128), BF16),
            pltpu.VMEM((64, 16, 128), BF16),
            pltpu.VMEM((2, 16, 4096), F32),
            pltpu.VMEM((2, 4, 2, 16, 512), BF16),
            pltpu.VMEM((2, 8, 16, 512), BF16),
            pltpu.VMEM((2, 16, 512), BF16),
            pltpu.VMEM((2, 8, 16, 512), BF16),
            pltpu.VMEM((64, 16, 128), BF16),
            pltpu.VMEM((16, 16, 128), BF16),
            pltpu.VMEM((16, 16, 128), BF16),
            pltpu.VMEM((32, 16, 128), BF16),
            pltpu.VMEM((3, 16, 16, 128), BF16),
            pltpu.VMEM((64, 16, 128), BF16),
            dma(8), dma(8), dma(4), dma(4), dma(4), dma(1), dma(2), dma(2), dma(2),
            dma(1), dma(4), dma(1), dma(8), dma(1), dma(2), dma(1), dma(2), dma(1), dma(1), dma(1),
            dma(2), dma(1), dma(2), dma(4), dma(4),
        ],
        compiler_params=pltpu.CompilerParams(
            collective_id=0, has_side_effects=True, vmem_limit_bytes=60 << 20
        ),
    )(
        order.reshape(1, -1), band_gain.reshape(1, -1), anomalies, alpha, basis, gradient,
        vertical_root, band.reshape(1, -1),
    )
    inc = pltpu.with_memory_space_constraint(inc, pltpu.VMEM)
    ag = pltpu.with_memory_space_constraint(ag, pltpu.VMEM)
    return pl.pallas_call(
        write_out,
        out_shape=(
            jax.ShapeDtypeStruct((32, 4096), F32),
            jax.ShapeDtypeStruct((16, 32, 128), F32),
        ),
        in_specs=[vmem] * 2,
        out_specs=(hbm, hbm),
        scratch_shapes=[dma(2)],
    )(inc, ag)


def solution(mesh):
    return jax.shard_map(
        on_device,
        mesh=mesh,
        in_specs=(
            P("mem", None, "state"),
            P("mem", None, "state"),
            P(None, "state"),
            P(None, "state"),
            P(),
            P(),
            P("state"),
            P(),
        ),
        out_specs=(P(None, "state"), P("mem", None, "state")),
        check_vma=False,
    )
```
